32 devices in a mesh: blk: 8 (over y, x, core), org: 4 (over z).
Axes of the slice: x: 2, y: 2, z: 4, core: 2. Of those that a mesh axis runs over, the one named last changes fastest.
Arguments:
- warm_labels: float32 [64, 512, 1024], P('blk', None, 'org'), may hold values from 0 to 6
- link_costs: float32 [4, 64, 512], P(None, 'blk'), may hold values from 0.05 to 1.5
- anchor_nodes: int32 [1024], P('org'), may hold values from 0 to 32767
- demand: float32 [1024], P('org'), may hold values from 0.2 to 2
Outputs:
- labels: float32 [64, 512, 1024], P('blk', None, 'org')
- link_weights: float32 [4, 64, 512], P(None, 'blk', 'org')
The draws below stay inside these ranges and needn't reach their ends.
Inputs may be any that keep to these rules, and one draw needn't show every extreme that they name: `anchor_nodes`: node numbers r * 512 + c.
All inputs are finite; a program needn't handle non-finite values.
Results may differ from the reference program's by a relative error of at most 0.0003.
Values sent between devices are 32-bit elements; how exact they have to be, the bound alone decides.
A program may use at most 128 MiB of HBM per device.

```python
import math
import jax
import jax.numpy as jnp
from jax import lax

ROWS_DEV = 8
GCOLS = 512
ANCHORS = 1024
INNER = 2
ROUNDS = 3
NROWS = 64
NODES = 32768
N_BLK = 8


def place_ends(array, stream_key, smallest, high):
    longest = array.shape.index(max(array.shape))
    spots = []
    for shift in (0, 1):
        where = [jax.random.randint(jax.random.fold_in(stream_key, axis), (), 0, length) for axis, length in enumerate(array.shape)]
        where[longest] = (where[longest] + shift) % array.shape[longest]
        spots.append(tuple(where))
    return array.at[spots[0]].set(smallest).at[spots[1]].set(high)


def block_scale(rng, extent, cuts, smallest, top_value):
    level = 1.0
    for position, blocks in cuts:
        steps = jax.random.uniform(jax.random.fold_in(jax.random.fold_in(rng, 6), position), (blocks,), jnp.float32, smallest / len(cuts), top_value / len(cuts))
        level = level * jnp.repeat(jnp.exp(steps), extent[position] // blocks).reshape((-1,) + (1,) * (len(extent) - 1 - position))
    return level


def setup_inputs(seed: int = 0) -> dict:
    key_list = jax.random.split(jax.random.key(seed), 5)
    warm_labels = jnp.clip(6.0 * jax.random.uniform(key_list[0], (NROWS, GCOLS, ANCHORS), jnp.float32) ** block_scale(key_list[0], (NROWS, GCOLS, ANCHORS), ((0, 8), (2, 4)), -0.2, 0.2), 0.0, 6.0)
    link_costs = jnp.clip(jnp.exp(math.log(1.5) - 3.4011974 * jax.random.uniform(key_list[1], (4, NROWS, GCOLS), jnp.float32) ** block_scale(key_list[1], (4, NROWS, GCOLS), ((1, 8),), -0.2, 0.2)), 0.05, 1.5)
    anchor_nodes = place_ends(jax.random.randint(key_list[2], (ANCHORS,), 0, NODES), jax.random.fold_in(key_list[2], 1), 0, NODES - 1).astype(jnp.int32)
    demand = jnp.clip(jnp.exp(math.log(2.0) - 2.3025851 * jax.random.uniform(key_list[3], (ANCHORS,), jnp.float32) ** block_scale(key_list[3], (ANCHORS,), ((0, 4),), -0.2, 0.2)), 0.2, 2.0)
    return dict(warm_labels=warm_labels, link_costs=link_costs, anchor_nodes=anchor_nodes, demand=demand)


far_value = 1e9
temper = 0.5


def relax_step(padded, costs):
    centre = padded[1:-1]
    edge = jnp.full((centre.shape[0], 1, centre.shape[2]), far_value, centre.dtype)
    west = jnp.concatenate([edge, centre[:, :-1]], axis=1) + costs[0, 1:-1][:, :, None]
    east = jnp.concatenate([centre[:, 1:], edge], axis=1) + costs[1, 1:-1][:, :, None]
    north = padded[:-2] + costs[2, 1:-1][:, :, None]
    south = padded[2:] + costs[3, 1:-1][:, :, None]
    return jnp.minimum(jnp.minimum(jnp.minimum(centre, west), jnp.minimum(east, north)), south)


def link_terms(padded, labels, costs, weights):
    edge = jnp.full((labels.shape[0], 1, labels.shape[2]), far_value, labels.dtype)
    sides = (jnp.concatenate([edge, labels[:, :-1]], axis=1),
             jnp.concatenate([labels[:, 1:], edge], axis=1),
             padded[:-2], padded[2:])
    result = []
    for side in range(4):
        expo = jnp.exp(-temper * (sides[side] + costs[side][:, :, None] - labels))
        result.append(jnp.einsum("rco,o->rc", expo, weights, precision=lax.Precision.HIGHEST))
    return jnp.stack(result)


def reference(warm_labels, link_costs, anchor_nodes, demand):
    total_rows = ROWS_DEV * N_BLK
    node_ids = (jnp.arange(total_rows, dtype=jnp.int32)[:, None] * GCOLS
                + jnp.arange(GCOLS, dtype=jnp.int32)[None, :]).astype(jnp.int32)
    block = 128 if ANCHORS % 128 == 0 else ANCHORS
    blocks = ANCHORS // block
    warm_blocks = warm_labels.reshape(total_rows, GCOLS, blocks, block).transpose(2, 0, 1, 3)
    cost_pad = jnp.pad(link_costs, ((0, 0), (1, 1), (0, 0)))

    def one_block(packed):
        warm, anchors, weights = packed
        labels = jnp.where(node_ids[:, :, None] == anchors[None, None, :], jnp.zeros_like(warm), warm)
        for sweep in range(ROUNDS * INNER):
            padded = jnp.pad(labels, ((1, 1), (0, 0), (0, 0)), constant_values=far_value)
            labels = relax_step(padded, cost_pad)
        padded = jnp.pad(labels, ((1, 1), (0, 0), (0, 0)), constant_values=far_value)
        return labels, link_terms(padded, labels, link_costs, weights)

    label_blocks, partials = lax.map(one_block, (warm_blocks, anchor_nodes.reshape(blocks, block),
                                                 demand.reshape(blocks, block)))
    labels = label_blocks.transpose(1, 2, 0, 3).reshape(total_rows, GCOLS, ANCHORS)
    link_weights = jnp.sum(partials, axis=0) / ANCHORS
    return labels, link_weights
```

```python
import functools
import math

import jax
import jax.numpy as jnp
from jax import lax
from jax.experimental import pallas as pl
from jax.experimental.pallas import tpu as pltpu
from jax.sharding import PartitionSpec as P

INNER = 2
ROUNDS = 3
STEPS = INNER * ROUNDS
HALO = STEPS + 1

far_value = 1000000000.0
temper = 0.5
RATE = temper * math.log2(math.e)
LANES = 128
PAD = 8
CHUNK = 32
BAND = 64
SPAN = 256
MESH = pl.DeviceIdType.MESH


def kernel(n, m, rows, cols, halves, warm, costs, anchors, demand, final, weights, grid, wide, raw, turned, decay, growth, tail,
           relay, sums, share, landed, near_out, near_in, row_send, row_recv, relay_in, relay_out, cost_send, cost_recv,
           org_send, org_recv, near_send, near_recv, local_sem):
    me = lax.axis_index("blk")
    org = lax.axis_index("org")
    has_top = me > 0
    has_bottom = me < n - 1
    top = jnp.maximum(me - 1, 0)
    bottom = jnp.minimum(me + 1, n - 1)
    first, last = HALO, HALO + rows - 1
    total = rows + 2 * HALO
    inner = pl.ds(PAD, cols)
    sides = ((has_top, top), (has_bottom, bottom))
    mid = n // 2
    relayed = n == 8
    via = (0, n - 1)
    goal = (mid - 1, mid)
    splits = tuple(relayed and me == goal[1 - side] for side in range(2))
    cut = cols // 2
    width = cols // m
    late = lax.rem(me, 2)
    early = 1 - late
    last_unit = STEPS * halves

    barrier = pltpu.get_barrier_semaphore()
    for there, who in sides:
        @pl.when(there)
        def _():
            for p in range(m):
                pl.semaphore_signal(barrier, inc=1, device_id={"blk": who, "org": p}, device_id_type=MESH)
    for d in range(1, m):
        pl.semaphore_signal(barrier, inc=1, device_id={"org": lax.rem(org + d, m)}, device_id_type=MESH)
    if relayed:
        for a, b in ((mid - 1, 0), (mid - 1, n - 1), (mid, 0), (mid, n - 1)):
            for mine, other in ((a, b), (b, a)):
                @pl.when(me == mine)
                def _():
                    pl.semaphore_signal(barrier, inc=1, device_id={"blk": other}, device_id_type=MESH)
    own_cost = pltpu.make_async_copy(costs, raw.at[0], local_sem.at[halves])
    own_cost.start()

    def own_rows(h):
        return pltpu.make_async_copy(
            warm.at[:, :, pl.ds(h * LANES, LANES)],
            grid.at[0, h, pl.ds(first, rows), inner, :],
            local_sem.at[h])
    for h in range(halves):
        own_rows(h).start()
    pl.semaphore_wait(barrier, m - 1 + jnp.where(has_top, m, 0) + jnp.where(has_bottom, m, 0)
                      + (jnp.where((me == 0) | (me == n - 1) | (me == mid) | (me == mid - 1), 2, 0) if relayed else 0))

    def cost_copy(side):
        return pltpu.make_async_remote_copy(
            src_ref=costs, dst_ref=raw.at[2 - side], send_sem=cost_send.at[side], recv_sem=cost_recv.at[side],
            device_id={"blk": sides[side][1]}, device_id_type=MESH)

    def source(side, j, h, start, count):
        row = jnp.where(side == 0, j - 1, rows - j)
        return warm.at[row, pl.ds(start, count), pl.ds(h * LANES, LANES)]

    def target(side, j, h, start, count):
        if isinstance(j, int) and j == HALO:
            return tail.at[1 - side, pl.ds(start, count), :]
        row = jnp.where(side == 0, last + j, first - j)
        return grid.at[0, h, row, pl.ds(PAD + start, count), :]

    def unit(j, h):
        return last_unit if isinstance(j, int) and j == HALO else (j - 1) * halves + h

    def row_copy(side, j, h, count):
        u = unit(j, h)
        return pltpu.make_async_remote_copy(
            src_ref=source(side, j, h, 0, count), dst_ref=target(side, j, h, 0, count),
            send_sem=row_send.at[side, u, 0], recv_sem=row_recv.at[side, u, 0],
            device_id={"blk": jnp.where(side == 0, top, bottom)}, device_id_type=MESH)

    def to_relay(side, j, h):
        u = unit(j, h)
        return pltpu.make_async_remote_copy(
            src_ref=source(side, j, h, cut, cols - cut), dst_ref=relay.at[u],
            send_sem=row_send.at[side, u, 1], recv_sem=relay_in.at[u],
            device_id={"blk": via[side]}, device_id_type=MESH)

    def from_relay(side, j, h):
        u = unit(j, h)
        return pltpu.make_async_remote_copy(
            src_ref=relay.at[u], dst_ref=target(side, j, h, cut, cols - cut),
            send_sem=relay_out.at[u], recv_sem=row_recv.at[side, u, 1],
            device_id={"blk": goal[side]}, device_id_type=MESH)

    def each_send(j, h, side, act):
        there, split = sides[side][0], splits[side]
        @pl.when(there & jnp.logical_not(split) if relayed else there)
        def _():
            act(row_copy(side, j, h, cols))
        if relayed:
            @pl.when(split)
            def _():
                act(to_relay(side, j, h))
                act(row_copy(side, j, h, cut))

    def all_sends(act):
        def body(j, carry):
            for h in range(halves):
                for side in range(2):
                    each_send(j, h, side, act)
            return carry
        lax.fori_loop(1, STEPS + 1, body, 0)
        for side in range(2):
            each_send(HALO, 1 - side, side, act)

    def arrive(halo, j, h):
        side = 1 - halo
        there = jnp.where(halo == 0, has_top, has_bottom)
        split = jnp.where(halo == 0, me == goal[1], me == goal[0]) & there
        @pl.when(there & jnp.logical_not(split) if relayed else there)
        def _():
            pltpu.make_async_remote_copy(
                src_ref=source(0, 1, 0, 0, cols), dst_ref=target(side, j, h, 0, cols),
                send_sem=row_send.at[side, unit(j, h), 0], recv_sem=row_recv.at[side, unit(j, h), 0],
                device_id={"blk": bottom}, device_id_type=MESH).wait_recv()
        if relayed:
            @pl.when(split)
            def _():
                for part, start, count in ((0, 0, cut), (1, cut, cols - cut)):
                    pltpu.make_async_remote_copy(
                        src_ref=source(0, 1, 0, start, count), dst_ref=target(side, j, h, start, count),
                        send_sem=row_send.at[side, unit(j, h), part], recv_sem=row_recv.at[side, unit(j, h), part],
                        device_id={"blk": bottom}, device_id_type=MESH).wait_recv()

    def forward(j, h):
        if relayed:
            for side in range(2):
                @pl.when(me == via[side])
                def _():
                    k = 1 - side if h is None else h
                    to_relay(side, j, k).wait_recv()
                    from_relay(side, j, k).start()

    for side in range(2):
        @pl.when(sides[side][0])
        def _():
            cost_copy(side).start()
    all_sends(lambda copy: copy.start())

    edge = jnp.full((PAD, LANES), far_value, jnp.float32)
    zero_edge = jnp.zeros((PAD, LANES), jnp.float32)

    def fill_edges(r, carry):
        for b in range(2):
            for h in range(halves):
                grid[b, h, r, pl.ds(0, PAD), :] = edge
                grid[b, h, r, pl.ds(PAD + cols, PAD), :] = edge
        return carry
    lax.fori_loop(0, total, fill_edges, 0)

    def fill_decay(r, carry):
        for h in range(halves):
            decay[h, r, pl.ds(0, PAD), :] = zero_edge
            decay[h, r, pl.ds(PAD + cols, PAD), :] = zero_edge
        return carry
    lax.fori_loop(0, rows + 2, fill_decay, 0)
    sums[...] = jnp.zeros_like(sums)
    raw[3] = jnp.zeros_like(raw[3])

    def fill_row(r):
        for h in range(halves):
            grid[0, h, r, inner, :] = jnp.full((cols, LANES), far_value, jnp.float32)
    fill_row(0)
    fill_row(total - 1)
    for missing, block, begin in ((me == 0, 1, 1), (me == n - 1, 2, last + 1)):
        @pl.when(missing)
        def _():
            raw[block] = jnp.full(raw.shape[1:], far_value, jnp.float32)
            def fill(r, carry):
                fill_row(begin + r)
                return carry
            lax.fori_loop(0, STEPS, fill, 0)

    def place(r):
        base = (me * rows + r - first) * cols
        names = [anchors[h] for h in range(halves)]
        for i in range(cols // CHUNK):
            node = lax.broadcasted_iota(jnp.int32, (CHUNK, LANES), 0) + (base + i * CHUNK)
            at = pl.ds(PAD + i * CHUNK, CHUNK)
            for h in range(halves):
                grid[0, h, r, at, :] = jnp.where(node == names[h], 0.0, grid[0, h, r, at, :])

    for h in range(halves):
        own_rows(h).wait()

    def place_own(r, carry):
        place(r)
        return carry
    lax.fori_loop(first, last + 1, place_own, 0)

    own_cost.wait()
    for side in range(2):
        @pl.when(sides[1 - side][0])
        def _():
            cost_copy(side).wait_recv()
    turned[...] = jnp.transpose(raw[...].reshape(4 * 4 * rows, cols))

    def widen(i, carry):
        at = pl.ds(pl.multiple_of(i * BAND, BAND), BAND)
        piece = turned[at, :]
        for r in range(1, total - 1):
            if r < first:
                block, row = 1, rows - first + r
            elif r <= last:
                block, row = 0, r - first
            else:
                block, row = 2, r - last - 1
            for k in range(4):
                lane = (block * 4 + k) * rows + row
                wide[k, r - 1, at, :] = jnp.broadcast_to(piece[:, lane:lane + 1], (BAND, LANES))
        return carry
    lax.fori_loop(0, cols // BAND, widen, 0)

    def best_of(old, r, i, hs):
        c0 = PAD + i * CHUNK
        at, mine = pl.ds(c0, CHUNK), pl.ds(i * CHUNK, CHUNK)
        price = [wide[k, r - 1, mine, :] for k in range(4)]
        result = []
        for h in hs:
            best = grid[old, h, r, at, :]
            best = jnp.minimum(best, grid[old, h, r, pl.ds(c0 - 1, CHUNK), :] + price[0])
            best = jnp.minimum(best, grid[old, h, r, pl.ds(c0 + 1, CHUNK), :] + price[1])
            best = jnp.minimum(best, grid[old, h, r - 1, at, :] + price[2])
            best = jnp.minimum(best, grid[old, h, r + 1, at, :] + price[3])
            result.append(best)
        return at, mine, result

    def relax(r, s, hs):
        old, new = lax.rem(s + 1, 2), lax.rem(s, 2)
        for i in range(cols // CHUNK):
            at, _, result = best_of(old, r, i, hs)
            for h, best in zip(hs, result):
                grid[new, h, r, at, :] = best

    both = tuple(range(halves))

    def finish(halo, j):
        r = jnp.where(halo == 0, first - j + STEPS, last + j - STEPS)
        q = r - first
        wants = [demand[h] for h in both]
        for i in range(cols // CHUNK):
            at, mine, result = best_of((STEPS + 1) % 2, r, i, both)
            for h, best in zip(both, result):
                final[q, mine, pl.ds(h * LANES, LANES)] = best
                power = best * RATE
                decay[h, q + 1, at, :] = jnp.exp2(-power)
                growth[h, q + 1, mine, :] = wants[h] * jnp.exp2(power)

    middle = rows // 2
    for s in range(1, middle):
        def inside(r, carry):
            relax(r, jnp.int32(s), both)
            return carry
        lax.fori_loop(first + s, last - s + 1, inside, 0)

    def stage(halo, j):
        for h in both:
            arrive(halo, j, h)
        place(jnp.where(halo == 0, first - j, last + j))

        def diagonal(s, carry):
            relax(jnp.where(halo == 0, first - j + s, last + j - s), s, both)
            return carry
        lax.fori_loop(1, jnp.minimum(STEPS - 1, j + middle - 1) + 1, diagonal, 0)

    def pair(q):
        return jnp.where(q == 0, early, late)

    def opening(j, carry):
        for h in both:
            forward(j, h)

        def one(q, carry):
            stage(pair(q), j)
            return carry
        return lax.fori_loop(0, 2, one, carry)

    def closing(j, carry):
        for h in both:
            forward(j, h)

        def one(q, carry):
            stage(pair(q), j)
            finish(pair(q), j)
            return carry
        return lax.fori_loop(0, 2, one, carry)

    ones = jnp.ones((8, 2 * LANES), jnp.bfloat16)

    def link(own, other, shift, hs, store):
        for c in range(0, cols, SPAN):
            term = None
            for h in hs:
                piece = growth[h, own, pl.ds(c, SPAN), :] * decay[h, other, pl.ds(PAD + c + shift, SPAN), :]
                term = piece if term is None else term + piece
            high = term.astype(jnp.bfloat16)
            low = (term - high.astype(jnp.float32)).astype(jnp.bfloat16)
            part = lax.dot_general(ones, jnp.concatenate([high, low], axis=1), (((1,), (1,)), ((), ())),
                                   preferred_element_type=jnp.float32)
            store(pl.ds(c, SPAN), part[0:1])

    def add_link(k, r, row, shift, hs):
        def store(at, part):
            sums[k, pl.ds(r - first, 1), at] = part
        link(r - first + 1, row - first + 1, shift, hs, store)

    def along(r, carry):
        add_link(0, r, r, -1, both)
        add_link(1, r, r, 1, both)
        return carry

    def across(r, carry):
        add_link(3, r, r + 1, 0, both)
        add_link(2, r + 1, r, 0, both)
        return carry

    def outer(halo):
        r0 = jnp.where(halo == 0, first - HALO, last + HALO)
        step = jnp.where(halo == 0, 1, -1)

        def diagonal(s, carry):
            relax(r0 + step * s, s, (halo,))
            return carry
        lax.fori_loop(1, STEPS + 1, diagonal, 0)

    scale = 1.0 / (m * halves * LANES)

    def cross(halo):
        there = jnp.where(halo == 0, has_top, has_bottom)
        r0 = jnp.where(halo == 0, first - HALO, last + HALO)
        step = jnp.where(halo == 0, 1, -1)
        own = jnp.where(halo == 0, 1, rows)
        other = jnp.where(halo == 0, 0, rows + 1)
        arrive(halo, HALO, halo)

        @pl.when(there)
        def _():
            base = (me * rows + r0 - first) * cols
            names, wants = anchors[halo], demand[halo]
            for i in range(cols // CHUNK):
                at, mine = pl.ds(PAD + i * CHUNK, CHUNK), pl.ds(i * CHUNK, CHUNK)
                node = lax.broadcasted_iota(jnp.int32, (CHUNK, LANES), 0) + (base + i * CHUNK)
                value = jnp.where(node == names, 0.0, tail[halo, mine, :])
                for t in range(1, STEPS + 1):
                    value = value + wide[2 + halo, r0 + step * t - 1, mine, :]
                power = jnp.minimum(value, grid[STEPS % 2, halo, r0 + step * STEPS, at, :]) * RATE
                decay[halo, other, at, :] = jnp.exp2(-power)
                growth[halo, other, mine, :] = wants * jnp.exp2(power)

            def mine_store(at, part):
                sums[2 + halo, pl.ds(own - 1, 1), at] = part
            link(own, other, 0, (halo,), mine_store)

            def near_store(at, part):
                fee = raw[1 + halo, 3 - halo, pl.ds(jnp.where(halo == 0, rows - 1, 0), 1), at]
                value = part * jnp.exp(-temper * fee) * scale
                for c in range(0, at.size, width):
                    near_out[halo, (at.start + c) // width] = value[:, c:c + width]
            link(other, own, 0, (halo,), near_store)

    def near_copy(halo, p):
        return pltpu.make_async_remote_copy(
            src_ref=near_out.at[halo, p], dst_ref=near_in.at[1 - halo, org], send_sem=near_send.at[halo, p],
            recv_sem=near_recv.at[1 - halo, org], device_id={"blk": sides[halo][1], "org": p}, device_id_type=MESH)

    def near_wait(halo, p):
        pltpu.make_async_remote_copy(
            src_ref=near_out.at[halo, p], dst_ref=near_in.at[halo, p], send_sem=near_send.at[halo, p],
            recv_sem=near_recv.at[halo, p], device_id={"blk": sides[halo][1], "org": p}, device_id_type=MESH).wait_recv()

    lax.fori_loop(1, 3, opening, 0)
    lax.fori_loop(3, STEPS, closing, 0)
    for h in both:
        forward(STEPS, h)
    forward(HALO, None)

    def closing_side(q, carry):
        halo = pair(q)
        stage(halo, STEPS)
        finish(halo, STEPS)
        outer(halo)
        low = jnp.where(q == 0, jnp.where(late == 0, first + 1, first), jnp.where(late == 0, first, last))
        high = jnp.where(q == 0, jnp.where(late == 0, last, last - 1), jnp.where(late == 0, first, last))
        lax.fori_loop(low, high + 1, along, 0)
        low = jnp.where(q == 0, jnp.where(late == 0, first + 1, first), jnp.where(late == 0, first, last - 1))
        high = jnp.where(q == 0, jnp.where(late == 0, last - 1, last - 2), jnp.where(late == 0, first, last - 1))
        lax.fori_loop(low, high + 1, across, 0)
        cross(halo)
        return carry
    lax.fori_loop(0, 2, closing_side, 0)

    ours = sums[...] * jnp.exp(-temper * raw[0]) * scale
    for p in range(m):
        share[p] = ours[:, :, p * width:(p + 1) * width]

    def org_copy(d):
        peer = lax.rem(org + d, m)
        return pltpu.make_async_remote_copy(
            src_ref=share.at[peer], dst_ref=landed.at[d - 1], send_sem=org_send.at[d - 1], recv_sem=org_recv.at[d - 1],
            device_id={"org": peer}, device_id_type=MESH)
    for halo in range(2):
        @pl.when(sides[halo][0])
        def _():
            for p in range(m):
                near_copy(halo, p).start()
    for d in range(1, m):
        org_copy(d).start()
    result = share[org]
    for d in range(1, m):
        org_copy(d).wait_recv()
        result += landed[d - 1]
    weights[...] = result
    for halo in range(2):
        @pl.when(sides[halo][0])
        def _():
            at = 0 if halo == 0 else rows - 1
            extra = weights[2 + halo, pl.ds(at, 1), :]
            for p in range(m):
                near_wait(halo, p)
                extra += near_in[halo, p]
            weights[2 + halo, pl.ds(at, 1), :] = extra

    for d in range(1, m):
        org_copy(d).wait_send()
    for side in range(2):
        @pl.when(sides[side][0])
        def _():
            cost_copy(side).wait_send()
            for p in range(m):
                near_copy(side, p).wait_send()
    all_sends(lambda copy: copy.wait_send())
    if relayed:
        for side in range(2):
            @pl.when(me == via[side])
            def _():
                def body(j, carry):
                    for h in both:
                        from_relay(side, j, h).wait_send()
                    return carry
                lax.fori_loop(1, STEPS + 1, body, 0)
                from_relay(side, HALO, 1 - side).wait_send()


def leave(rows, labels, weights, labels_out, weights_out, sems):
    copies = [pltpu.make_async_copy(labels.at[r], labels_out.at[r], sems.at[r]) for r in range(rows)]
    copies.append(pltpu.make_async_copy(weights, weights_out, sems.at[rows]))
    for copy in copies:
        copy.start()
    for copy in copies:
        copy.wait()


def local(n, m, warm_labels, link_costs, anchor_nodes, demand):
    rows, cols, count = warm_labels.shape
    halves = count // LANES
    total = rows + 2 * HALO
    width = cols // m
    units = STEPS * halves + 1
    any_space = pl.BlockSpec(memory_space=pl.ANY)
    vmem = pl.BlockSpec(memory_space=pltpu.VMEM)
    dma = pltpu.SemaphoreType.DMA
    labels, weights = pl.pallas_call(
        functools.partial(kernel, n, m, rows, cols, halves),
        out_shape=(
            pltpu.VMEM((rows, cols, count), jnp.float32),
            pltpu.VMEM((4, rows, width), jnp.float32),
        ),
        in_specs=[any_space, any_space, vmem, vmem],
        out_specs=(vmem, vmem),
        scratch_shapes=[
            pltpu.VMEM((2, halves, total, cols + 2 * PAD, LANES), jnp.float32),
            pltpu.VMEM((4, total - 2, cols, LANES), jnp.float32),
            pltpu.VMEM((4, 4, rows, cols), jnp.float32),
            pltpu.VMEM((cols, 16 * rows), jnp.float32),
            pltpu.VMEM((halves, rows + 2, cols + 2 * PAD, LANES), jnp.float32),
            pltpu.VMEM((halves, rows + 2, cols, LANES), jnp.float32),
            pltpu.VMEM((2, cols, LANES), jnp.float32),
            pltpu.VMEM((units, cols - cols // 2, LANES), jnp.float32),
            pltpu.VMEM((4, rows, cols), jnp.float32),
            pltpu.VMEM((m, 4, rows, width), jnp.float32),
            pltpu.VMEM((max(m - 1, 1), 4, rows, width), jnp.float32),
            pltpu.VMEM((2, m, 1, width), jnp.float32),
            pltpu.VMEM((2, m, 1, width), jnp.float32),
            dma((2, units, 2)),
            dma((2, units, 2)),
            dma((units,)),
            dma((units,)),
            dma((2,)),
            dma((2,)),
            dma((max(m - 1, 1),)),
            dma((max(m - 1, 1),)),
            dma((2, m)),
            dma((2, m)),
            dma((halves + 1,)),
        ],
        compiler_params=pltpu.CompilerParams(collective_id=0, has_side_effects=True, vmem_limit_bytes=58 * 1024 * 1024),
    )(warm_labels, link_costs, anchor_nodes.reshape(halves, 1, LANES), demand.reshape(halves, 1, LANES))
    labels = pltpu.with_memory_space_constraint(labels, pltpu.VMEM)
    weights = pltpu.with_memory_space_constraint(weights, pltpu.VMEM)
    return pl.pallas_call(
        functools.partial(leave, rows),
        out_shape=(
            jax.ShapeDtypeStruct((rows, cols, count), jnp.float32),
            jax.ShapeDtypeStruct((4, rows, width), jnp.float32),
        ),
        in_specs=[vmem, vmem],
        out_specs=(any_space, any_space),
        scratch_shapes=[dma((rows + 1,))],
        compiler_params=pltpu.CompilerParams(vmem_limit_bytes=8 * 1024 * 1024),
    )(labels, weights)


def solution(mesh):
    placed = (P("blk", None, "org"), P(None, "blk", None), P("org"), P("org"))
    return jax.shard_map(
        functools.partial(local, mesh.shape["blk"], mesh.shape["org"]),
        mesh=mesh,
        in_specs=placed,
        out_specs=(P("blk", None, "org"), P(None, "blk", "org")),
        check_vma=False,
    )
```

```python
import functools
import math

import jax
import jax.numpy as jnp
from jax import lax
from jax.experimental import pallas as pl
from jax.experimental.pallas import tpu as pltpu
from jax.sharding import PartitionSpec as P

INNER = 2
ROUNDS = 3
STEPS = INNER * ROUNDS
HALO = STEPS + 1

far_value = 1000000000.0
temper = 0.5
RATE = temper * math.log2(math.e)
LANES = 128
PAD = 8
CHUNK = 32
BAND = 64
SPAN = 256
MESH = pl.DeviceIdType.MESH


def kernel(n, m, rows, cols, halves, warm, costs, anchors, demand, final, weights, grid, wide, raw, turned, decay, growth, tail,
           relay, sums, share, landed, near_out, near_in, row_send, row_recv, relay_in, relay_out, cost_send, cost_recv,
           org_send, org_recv, near_send, near_recv, local_sem):
    me = lax.axis_index("blk")
    org = lax.axis_index("org")
    has_top = me > 0
    has_bottom = me < n - 1
    top = jnp.maximum(me - 1, 0)
    bottom = jnp.minimum(me + 1, n - 1)
    first, last = HALO, HALO + rows - 1
    total = rows + 2 * HALO
    inner = pl.ds(PAD, cols)
    sides = ((has_top, top), (has_bottom, bottom))
    mid = n // 2
    relayed = n == 8
    via = (0, n - 1)
    goal = (mid - 1, mid)
    splits = tuple(relayed and me == goal[1 - side] for side in range(2))
    cut = cols // 2
    width = cols // m
    late = lax.rem(me, 2)
    early = 1 - late
    last_unit = STEPS * halves

    barrier = pltpu.get_barrier_semaphore()
    for there, who in sides:
        @pl.when(there)
        def _():
            for p in range(m):
                pl.semaphore_signal(barrier, inc=1, device_id={"blk": who, "org": p}, device_id_type=MESH)
    for d in range(1, m):
        pl.semaphore_signal(barrier, inc=1, device_id={"org": lax.rem(org + d, m)}, device_id_type=MESH)
    if relayed:
        for a, b in ((mid - 1, 0), (mid - 1, n - 1), (mid, 0), (mid, n - 1)):
            for mine, other in ((a, b), (b, a)):
                @pl.when(me == mine)
                def _():
                    pl.semaphore_signal(barrier, inc=1, device_id={"blk": other}, device_id_type=MESH)
    own_cost = pltpu.make_async_copy(costs, raw.at[0], local_sem.at[halves])
    own_cost.start()

    def own_rows(h):
        return pltpu.make_async_copy(
            warm.at[:, :, pl.ds(h * LANES, LANES)],
            grid.at[0, h, pl.ds(first, rows), inner, :],
            local_sem.at[h])
    for h in range(halves):
        own_rows(h).start()
    pl.semaphore_wait(barrier, m - 1 + jnp.where(has_top, m, 0) + jnp.where(has_bottom, m, 0)
                      + (jnp.where((me == 0) | (me == n - 1) | (me == mid) | (me == mid - 1), 2, 0) if relayed else 0))

    part = 4 // m
    piece_of = pl.ds(org * part, part)

    def cost_copy(side):
        return pltpu.make_async_remote_copy(
            src_ref=costs.at[piece_of], dst_ref=raw.at[2 - side, piece_of], send_sem=cost_send.at[side, 0],
            recv_sem=cost_recv.at[side, 0], device_id={"blk": sides[side][1]}, device_id_type=MESH)

    def cost_spread(side, d):
        return pltpu.make_async_remote_copy(
            src_ref=raw.at[2 - side, piece_of], dst_ref=raw.at[2 - side, piece_of], send_sem=cost_send.at[side, d],
            recv_sem=cost_recv.at[side, d], device_id={"org": lax.rem(org + d, m)}, device_id_type=MESH)

    def source(side, j, h, start, count):
        row = jnp.where(side == 0, j - 1, rows - j)
        return warm.at[row, pl.ds(start, count), pl.ds(h * LANES, LANES)]

    def target(side, j, h, start, count):
        if isinstance(j, int) and j >= STEPS:
            return tail.at[1 - side, halves if j == HALO else h, pl.ds(start, count), :]
        row = jnp.where(side == 0, last + j, first - j)
        return grid.at[0, h, row, pl.ds(PAD + start, count), :]

    def unit(j, h):
        return last_unit if isinstance(j, int) and j == HALO else (j - 1) * halves + h

    def row_copy(side, j, h, count):
        u = unit(j, h)
        return pltpu.make_async_remote_copy(
            src_ref=source(side, j, h, 0, count), dst_ref=target(side, j, h, 0, count),
            send_sem=row_send.at[side, u, 0], recv_sem=row_recv.at[side, u, 0],
            device_id={"blk": jnp.where(side == 0, top, bottom)}, device_id_type=MESH)

    def to_relay(side, j, h):
        u = unit(j, h)
        return pltpu.make_async_remote_copy(
            src_ref=source(side, j, h, cut, cols - cut), dst_ref=relay.at[u],
            send_sem=row_send.at[side, u, 1], recv_sem=relay_in.at[u],
            device_id={"blk": via[side]}, device_id_type=MESH)

    def from_relay(side, j, h):
        u = unit(j, h)
        return pltpu.make_async_remote_copy(
            src_ref=relay.at[u], dst_ref=target(side, j, h, cut, cols - cut),
            send_sem=relay_out.at[u], recv_sem=row_recv.at[side, u, 1],
            device_id={"blk": goal[side]}, device_id_type=MESH)

    def each_send(j, h, side, act):
        there, split = sides[side][0], splits[side]
        @pl.when(there & jnp.logical_not(split) if relayed else there)
        def _():
            act(row_copy(side, j, h, cols))
        if relayed:
            @pl.when(split)
            def _():
                act(to_relay(side, j, h))
                act(row_copy(side, j, h, cut))

    def all_sends(act):
        def body(j, carry):
            for h in range(halves):
                for side in range(2):
                    each_send(j, h if side else halves - 1 - h, side, act)
            return carry
        lax.fori_loop(1, STEPS, body, 0)
        body(STEPS, 0)
        for side in range(2):
            each_send(HALO, 1 - side, side, act)

    def arrive(halo, j, h):
        side = 1 - halo
        there = jnp.where(halo == 0, has_top, has_bottom)
        split = jnp.where(halo == 0, me == goal[1], me == goal[0]) & there
        @pl.when(there & jnp.logical_not(split) if relayed else there)
        def _():
            pltpu.make_async_remote_copy(
                src_ref=source(0, 1, 0, 0, cols), dst_ref=target(side, j, h, 0, cols),
                send_sem=row_send.at[side, unit(j, h), 0], recv_sem=row_recv.at[side, unit(j, h), 0],
                device_id={"blk": bottom}, device_id_type=MESH).wait_recv()
        if relayed:
            @pl.when(split)
            def _():
                for part, start, count in ((0, 0, cut), (1, cut, cols - cut)):
                    pltpu.make_async_remote_copy(
                        src_ref=source(0, 1, 0, start, count), dst_ref=target(side, j, h, start, count),
                        send_sem=row_send.at[side, unit(j, h), part], recv_sem=row_recv.at[side, unit(j, h), part],
                        device_id={"blk": bottom}, device_id_type=MESH).wait_recv()

    def forward(j):
        if relayed:
            for side in range(2):
                @pl.when(me == via[side])
                def _():
                    for h in (1 - side, side)[:1 if isinstance(j, int) and j == HALO else 2]:
                        to_relay(side, j, h).wait_recv()
                        from_relay(side, j, h).start()

    for side in range(2):
        @pl.when(sides[side][0])
        def _():
            cost_copy(side).start()
    all_sends(lambda copy: copy.start())

    edge = jnp.full((PAD, LANES), far_value, jnp.float32)
    zero_edge = jnp.zeros((PAD, LANES), jnp.float32)

    def fill_edges(r, carry):
        for b in range(2):
            for h in range(halves):
                grid[b, h, r, pl.ds(0, PAD), :] = edge
                grid[b, h, r, pl.ds(PAD + cols, PAD), :] = edge
        return carry
    lax.fori_loop(0, total, fill_edges, 0)

    def fill_decay(r, carry):
        for h in range(halves):
            decay[h, r, pl.ds(0, PAD), :] = zero_edge
            decay[h, r, pl.ds(PAD + cols, PAD), :] = zero_edge
        return carry
    lax.fori_loop(0, rows + 2, fill_decay, 0)
    sums[...] = jnp.zeros_like(sums)
    raw[3] = jnp.zeros_like(raw[3])

    def fill_row(r):
        for h in range(halves):
            grid[0, h, r, inner, :] = jnp.full((cols, LANES), far_value, jnp.float32)
    for r in (0, 1, total - 2, total - 1):
        fill_row(r)
    for missing, block, begin in ((me == 0, 1, 2), (me == n - 1, 2, last + 1)):
        @pl.when(missing)
        def _():
            raw[block] = jnp.full(raw.shape[1:], far_value, jnp.float32)
            def fill(r, carry):
                fill_row(begin + r)
                return carry
            lax.fori_loop(0, STEPS - 1, fill, 0)

    def place(r):
        base = (me * rows + r - first) * cols
        names = [anchors[h] for h in range(halves)]
        for i in range(cols // CHUNK):
            node = lax.broadcasted_iota(jnp.int32, (CHUNK, LANES), 0) + (base + i * CHUNK)
            at = pl.ds(PAD + i * CHUNK, CHUNK)
            for h in range(halves):
                grid[0, h, r, at, :] = jnp.where(node == names[h], 0.0, grid[0, h, r, at, :])

    for side in range(2):
        @pl.when(sides[1 - side][0])
        def _():
            cost_copy(side).wait_recv()
            for d in range(1, m):
                cost_spread(side, d).start()

    for h in range(halves):
        own_rows(h).wait()

    def place_own(r, carry):
        place(r)
        return carry
    lax.fori_loop(first, last + 1, place_own, 0)

    own_cost.wait()
    for side in range(2):
        @pl.when(sides[1 - side][0])
        def _():
            for d in range(1, m):
                cost_spread(side, d).wait_recv()
    turned[...] = jnp.transpose(raw[...].reshape(4 * 4 * rows, cols))

    def widen(i, carry):
        at = pl.ds(pl.multiple_of(i * BAND, BAND), BAND)
        piece = turned[at, :]
        for r in range(1, total - 1):
            if r < first:
                block, row = 1, rows - first + r
            elif r <= last:
                block, row = 0, r - first
            else:
                block, row = 2, r - last - 1
            for k in range(4):
                lane = (block * 4 + k) * rows + row
                wide[k, r - 1, at, :] = jnp.broadcast_to(piece[:, lane:lane + 1], (BAND, LANES))
        return carry
    lax.fori_loop(0, cols // BAND, widen, 0)

    def best_of(old, r, i, hs):
        c0 = PAD + i * CHUNK
        at, mine = pl.ds(c0, CHUNK), pl.ds(i * CHUNK, CHUNK)
        price = [wide[k, r - 1, mine, :] for k in range(4)]
        result = []
        for h in hs:
            best = grid[old, h, r, at, :]
            best = jnp.minimum(best, grid[old, h, r, pl.ds(c0 - 1, CHUNK), :] + price[0])
            best = jnp.minimum(best, grid[old, h, r, pl.ds(c0 + 1, CHUNK), :] + price[1])
            best = jnp.minimum(best, grid[old, h, r - 1, at, :] + price[2])
            best = jnp.minimum(best, grid[old, h, r + 1, at, :] + price[3])
            result.append(best)
        return at, mine, result

    def relax(r, s, hs):
        old, new = lax.rem(s + 1, 2), lax.rem(s, 2)
        for i in range(cols // CHUNK):
            at, _, result = best_of(old, r, i, hs)
            for h, best in zip(hs, result):
                grid[new, h, r, at, :] = best

    both = tuple(range(halves))

    def finish(halo, j):
        r = jnp.where(halo == 0, first - j + STEPS, last + j - STEPS)
        q = r - first
        wants = [demand[h] for h in both]
        for i in range(cols // CHUNK):
            at, mine, result = best_of((STEPS + 1) % 2, r, i, both)
            for h, best in zip(both, result):
                final[q, mine, pl.ds(h * LANES, LANES)] = best
                power = best * RATE
                decay[h, q + 1, at, :] = jnp.exp2(-power)
                growth[h, q + 1, mine, :] = wants[h] * jnp.exp2(power)

    middle = rows // 2
    for s in range(1, middle):
        def inside(r, carry):
            relax(r, jnp.int32(s), both)
            return carry
        lax.fori_loop(first + s, last - s + 1, inside, 0)

    def stage(halo, j):
        for h in both:
            arrive(halo, j, h)
        place(jnp.where(halo == 0, first - j, last + j))

        def diagonal(s, carry):
            relax(jnp.where(halo == 0, first - j + s, last + j - s), s, both)
            return carry
        lax.fori_loop(1, jnp.minimum(STEPS - 1, j + middle - 1) + 1, diagonal, 0)

    def pair(q):
        return jnp.where(q == 0, early, late)

    def opening(j, carry):
        forward(j)

        def one(q, carry):
            stage(pair(q), j)
            return carry
        return lax.fori_loop(0, 2, one, carry)

    def closing(j, carry):
        forward(j)

        def one(q, carry):
            stage(pair(q), j)
            finish(pair(q), j)
            return carry
        return lax.fori_loop(0, 2, one, carry)

    ones = jnp.ones((8, 2 * LANES), jnp.bfloat16)

    def link(own, other, shift, hs, store):
        for c in range(0, cols, SPAN):
            term = None
            for h in hs:
                piece = growth[h, own, pl.ds(c, SPAN), :] * decay[h, other, pl.ds(PAD + c + shift, SPAN), :]
                term = piece if term is None else term + piece
            high = term.astype(jnp.bfloat16)
            low = (term - high.astype(jnp.float32)).astype(jnp.bfloat16)
            part = lax.dot_general(ones, jnp.concatenate([high, low], axis=1), (((1,), (1,)), ((), ())),
                                   preferred_element_type=jnp.float32)
            store(pl.ds(c, SPAN), part[0:1])

    def add_link(k, r, row, shift, hs):
        def store(at, part):
            sums[k, pl.ds(r - first, 1), at] = part
        link(r - first + 1, row - first + 1, shift, hs, store)

    def along(r, carry):
        add_link(0, r, r, -1, both)
        add_link(1, r, r, 1, both)
        return carry

    def across(r, carry):
        add_link(3, r, r + 1, 0, both)
        add_link(2, r + 1, r, 0, both)
        return carry

    def outer(halo):
        r0 = jnp.where(halo == 0, first - HALO, last + HALO)
        step = jnp.where(halo == 0, 1, -1)

        def diagonal(s, carry):
            relax(r0 + step * s, s, (halo,))
            return carry
        lax.fori_loop(1, STEPS + 1, diagonal, 0)

    scale = 1.0 / (m * halves * LANES)

    def cross(halo):
        there = jnp.where(halo == 0, has_top, has_bottom)
        r0 = jnp.where(halo == 0, first - HALO, last + HALO)
        step = jnp.where(halo == 0, 1, -1)
        own = jnp.where(halo == 0, 1, rows)
        other = jnp.where(halo == 0, 0, rows + 1)
        arrive(halo, HALO, halo)

        @pl.when(there)
        def _():
            base = (me * rows + r0 - first) * cols
            names, wants = anchors[halo], demand[halo]
            for i in range(cols // CHUNK):
                at, mine = pl.ds(PAD + i * CHUNK, CHUNK), pl.ds(i * CHUNK, CHUNK)
                node = lax.broadcasted_iota(jnp.int32, (CHUNK, LANES), 0) + (base + i * CHUNK)
                value = jnp.where(node == names, 0.0, tail[halo, halves, mine, :])
                for t in range(1, STEPS + 1):
                    value = value + wide[2 + halo, r0 + step * t - 1, mine, :]
                power = jnp.minimum(value, grid[STEPS % 2, halo, r0 + step * STEPS, at, :]) * RATE
                decay[halo, other, at, :] = jnp.exp2(-power)
                growth[halo, other, mine, :] = wants * jnp.exp2(power)

            def mine_store(at, part):
                sums[2 + halo, pl.ds(own - 1, 1), at] = part
            link(own, other, 0, (halo,), mine_store)

            def near_store(at, part):
                fee = raw[1 + halo, 3 - halo, pl.ds(jnp.where(halo == 0, rows - 1, 0), 1), at]
                value = part * jnp.exp(-temper * fee) * scale
                for c in range(0, at.size, width):
                    near_out[halo, (at.start + c) // width] = value[:, c:c + width]
            link(other, own, 0, (halo,), near_store)

    def near_copy(halo, p):
        return pltpu.make_async_remote_copy(
            src_ref=near_out.at[halo, p], dst_ref=near_in.at[1 - halo, org], send_sem=near_send.at[halo, p],
            recv_sem=near_recv.at[1 - halo, org], device_id={"blk": sides[halo][1], "org": p}, device_id_type=MESH)

    def near_wait(halo, p):
        pltpu.make_async_remote_copy(
            src_ref=near_out.at[halo, p], dst_ref=near_in.at[halo, p], send_sem=near_send.at[halo, p],
            recv_sem=near_recv.at[halo, p], device_id={"blk": sides[halo][1], "org": p}, device_id_type=MESH).wait_recv()

    lax.fori_loop(1, 3, opening, 0)
    lax.fori_loop(3, STEPS, closing, 0)
    forward(STEPS)
    forward(HALO)

    def ahead(halo):
        def diagonal(s, carry):
            relax(jnp.where(halo == 0, first - STEPS + s, last + STEPS - s), s, both)
            return carry
        lax.fori_loop(1, STEPS + 1, diagonal, 0)

    def chain(halo, h):
        there = jnp.where(halo == 0, has_top, has_bottom)
        r0 = jnp.where(halo == 0, first - STEPS, last + STEPS)
        step = jnp.where(halo == 0, 1, -1)
        q = jnp.where(halo == 0, 0, rows - 1)
        arrive(halo, STEPS, h)

        @pl.when(there)
        def _():
            base = (me * rows + r0 - first) * cols
            for i in range(cols // CHUNK):
                at, mine = pl.ds(PAD + i * CHUNK, CHUNK), pl.ds(i * CHUNK, CHUNK)
                node = lax.broadcasted_iota(jnp.int32, (CHUNK, LANES), 0) + (base + i * CHUNK)
                value = jnp.where(node == anchors[h], 0.0, tail[halo, h, mine, :])
                grid[0, h, r0, at, :] = value
                for t in range(1, STEPS + 1):
                    r = r0 + step * t
                    value = jnp.minimum(grid[t % 2, h, r, at, :], value + wide[2 + halo, r - 1, mine, :])
                    grid[t % 2, h, r, at, :] = value

        def settle(h_static):
            for i in range(cols // CHUNK):
                at, mine = pl.ds(PAD + i * CHUNK, CHUNK), pl.ds(i * CHUNK, CHUNK)
                value = grid[STEPS % 2, h_static, q + first, at, :]
                final[q, mine, pl.ds(h_static * LANES, LANES)] = value
                power = value * RATE
                decay[h_static, q + 1, at, :] = jnp.exp2(-power)
                growth[h_static, q + 1, mine, :] = demand[h_static] * jnp.exp2(power)
        for k in both:
            @pl.when(h == k)
            def _():
                settle(k)

    def closing_side(q, carry):
        halo = pair(q)
        ahead(halo)
        chain(halo, halo)
        outer(halo)
        chain(halo, 1 - halo)
        low = jnp.where(q == 0, jnp.where(late == 0, first + 1, first), jnp.where(late == 0, first, last))
        high = jnp.where(q == 0, jnp.where(late == 0, last, last - 1), jnp.where(late == 0, first, last))
        lax.fori_loop(low, high + 1, along, 0)
        low = jnp.where(q == 0, jnp.where(late == 0, first + 1, first), jnp.where(late == 0, first, last - 1))
        high = jnp.where(q == 0, jnp.where(late == 0, last - 1, last - 2), jnp.where(late == 0, first, last - 1))
        lax.fori_loop(low, high + 1, across, 0)
        cross(halo)
        return carry
    lax.fori_loop(0, 2, closing_side, 0)

    ours = sums[...] * jnp.exp(-temper * raw[0]) * scale
    for p in range(m):
        share[p] = ours[:, :, p * width:(p + 1) * width]

    def org_copy(d):
        peer = lax.rem(org + d, m)
        return pltpu.make_async_remote_copy(
            src_ref=share.at[peer], dst_ref=landed.at[d - 1], send_sem=org_send.at[d - 1], recv_sem=org_recv.at[d - 1],
            device_id={"org": peer}, device_id_type=MESH)
    for halo in range(2):
        @pl.when(sides[halo][0])
        def _():
            for p in range(m):
                near_copy(halo, p).start()
    for d in range(1, m):
        org_copy(d).start()
    result = share[org]
    for d in range(1, m):
        org_copy(d).wait_recv()
        result += landed[d - 1]
    weights[...] = result
    for halo in range(2):
        @pl.when(sides[halo][0])
        def _():
            at = 0 if halo == 0 else rows - 1
            extra = weights[2 + halo, pl.ds(at, 1), :]
            for p in range(m):
                near_wait(halo, p)
                extra += near_in[halo, p]
            weights[2 + halo, pl.ds(at, 1), :] = extra

    for d in range(1, m):
        org_copy(d).wait_send()
    for side in range(2):
        @pl.when(sides[side][0])
        def _():
            cost_copy(side).wait_send()
            for p in range(m):
                near_copy(side, p).wait_send()
        @pl.when(sides[1 - side][0])
        def _():
            for d in range(1, m):
                cost_spread(side, d).wait_send()
    all_sends(lambda copy: copy.wait_send())
    if relayed:
        for side in range(2):
            @pl.when(me == via[side])
            def _():
                def body(j, carry):
                    for h in both:
                        from_relay(side, j, h).wait_send()
                    return carry
                lax.fori_loop(1, STEPS, body, 0)
                body(STEPS, 0)
                from_relay(side, HALO, 1 - side).wait_send()


def leave(rows, labels, weights, labels_out, weights_out, sems):
    copies = [pltpu.make_async_copy(labels.at[r], labels_out.at[r], sems.at[r]) for r in range(rows)]
    copies.append(pltpu.make_async_copy(weights, weights_out, sems.at[rows]))
    for copy in copies:
        copy.start()
    for copy in copies:
        copy.wait()


def local(n, m, warm_labels, link_costs, anchor_nodes, demand):
    rows, cols, count = warm_labels.shape
    halves = count // LANES
    total = rows + 2 * HALO
    width = cols // m
    units = STEPS * halves + 1
    any_space = pl.BlockSpec(memory_space=pl.ANY)
    vmem = pl.BlockSpec(memory_space=pltpu.VMEM)
    dma = pltpu.SemaphoreType.DMA
    labels, weights = pl.pallas_call(
        functools.partial(kernel, n, m, rows, cols, halves),
        out_shape=(
            pltpu.VMEM((rows, cols, count), jnp.float32),
            pltpu.VMEM((4, rows, width), jnp.float32),
        ),
        in_specs=[any_space, any_space, vmem, vmem],
        out_specs=(vmem, vmem),
        scratch_shapes=[
            pltpu.VMEM((2, halves, total, cols + 2 * PAD, LANES), jnp.float32),
            pltpu.VMEM((4, total - 2, cols, LANES), jnp.float32),
            pltpu.VMEM((4, 4, rows, cols), jnp.float32),
            pltpu.VMEM((cols, 16 * rows), jnp.float32),
            pltpu.VMEM((halves, rows + 2, cols + 2 * PAD, LANES), jnp.float32),
            pltpu.VMEM((halves, rows + 2, cols, LANES), jnp.float32),
            pltpu.VMEM((2, halves + 1, cols, LANES), jnp.float32),
            pltpu.VMEM((units, cols - cols // 2, LANES), jnp.float32),
            pltpu.VMEM((4, rows, cols), jnp.float32),
            pltpu.VMEM((m, 4, rows, width), jnp.float32),
            pltpu.VMEM((max(m - 1, 1), 4, rows, width), jnp.float32),
            pltpu.VMEM((2, m, 1, width), jnp.float32),
            pltpu.VMEM((2, m, 1, width), jnp.float32),
            dma((2, units, 2)),
            dma((2, units, 2)),
            dma((units,)),
            dma((units,)),
            dma((2, m)),
            dma((2, m)),
            dma((max(m - 1, 1),)),
            dma((max(m - 1, 1),)),
            dma((2, m)),
            dma((2, m)),
            dma((halves + 1,)),
        ],
        compiler_params=pltpu.CompilerParams(collective_id=0, has_side_effects=True, vmem_limit_bytes=58 * 1024 * 1024),
    )(warm_labels, link_costs, anchor_nodes.reshape(halves, 1, LANES), demand.reshape(halves, 1, LANES))
    labels = pltpu.with_memory_space_constraint(labels, pltpu.VMEM)
    weights = pltpu.with_memory_space_constraint(weights, pltpu.VMEM)
    return pl.pallas_call(
        functools.partial(leave, rows),
        out_shape=(
            jax.ShapeDtypeStruct((rows, cols, count), jnp.float32),
            jax.ShapeDtypeStruct((4, rows, width), jnp.float32),
        ),
        in_specs=[vmem, vmem],
        out_specs=(any_space, any_space),
        scratch_shapes=[dma((rows + 1,))],
        compiler_params=pltpu.CompilerParams(vmem_limit_bytes=8 * 1024 * 1024),
    )(labels, weights)


def solution(mesh):
    placed = (P("blk", None, "org"), P(None, "blk", None), P("org"), P("org"))
    return jax.shard_map(
        functools.partial(local, mesh.shape["blk"], mesh.shape["org"]),
        mesh=mesh,
        in_specs=placed,
        out_specs=(P("blk", None, "org"), P(None, "blk", "org")),
        check_vma=False,
    )
```

```python
import functools
import math

import jax
import jax.numpy as jnp
from jax import lax
from jax.experimental import pallas as pl
from jax.experimental.pallas import tpu as pltpu
from jax.sharding import PartitionSpec as P

INNER = 2
ROUNDS = 3
STEPS = INNER * ROUNDS
HALO = STEPS + 1

far_value = 1000000000.0
temper = 0.5
RATE = temper * math.log2(math.e)
LANES = 128
PAD = 8
CHUNK = 32
BAND = 64
SPAN = 256
MESH = pl.DeviceIdType.MESH


def kernel(n, m, rows, cols, halves, warm, costs, anchors, demand, final, weights, grid, wide, raw, turned, decay, growth, tail,
           relay, sums, share, landed, near_out, near_in, row_send, row_recv, relay_in, relay_out, cost_send, cost_recv,
           org_send, org_recv, near_send, near_recv, local_sem):
    me = lax.axis_index("blk")
    org = lax.axis_index("org")
    has_top = me > 0
    has_bottom = me < n - 1
    top = jnp.maximum(me - 1, 0)
    bottom = jnp.minimum(me + 1, n - 1)
    first, last = HALO, HALO + rows - 1
    total = rows + 2 * HALO
    inner = pl.ds(PAD, cols)
    sides = ((has_top, top), (has_bottom, bottom))
    mid = n // 2
    relayed = n == 8
    via = (0, n - 1)
    goal = (mid - 1, mid)
    splits = tuple(relayed and me == goal[1 - side] for side in range(2))
    cut = cols // 2
    width = cols // m
    late = lax.rem(me, 2)
    early = 1 - late
    last_unit = STEPS * halves

    barrier = pltpu.get_barrier_semaphore()
    for there, who in sides:
        @pl.when(there)
        def _():
            for p in range(m):
                pl.semaphore_signal(barrier, inc=1, device_id={"blk": who, "org": p}, device_id_type=MESH)
    for d in range(1, m):
        pl.semaphore_signal(barrier, inc=1, device_id={"org": lax.rem(org + d, m)}, device_id_type=MESH)
    if relayed:
        for a, b in ((mid - 1, 0), (mid - 1, n - 1), (mid, 0), (mid, n - 1)):
            for mine, other in ((a, b), (b, a)):
                @pl.when(me == mine)
                def _():
                    pl.semaphore_signal(barrier, inc=1, device_id={"blk": other}, device_id_type=MESH)
    own_cost = pltpu.make_async_copy(costs, raw.at[0], local_sem.at[halves])
    own_cost.start()

    def own_rows(h):
        return pltpu.make_async_copy(
            warm.at[:, :, pl.ds(h * LANES, LANES)],
            grid.at[0, h, pl.ds(first, rows), inner, :],
            local_sem.at[h])
    for h in range(halves):
        own_rows(h).start()
    pl.semaphore_wait(barrier, m - 1 + jnp.where(has_top, m, 0) + jnp.where(has_bottom, m, 0)
                      + (jnp.where((me == 0) | (me == n - 1) | (me == mid) | (me == mid - 1), 2, 0) if relayed else 0))

    part = 4 // m
    piece_of = pl.ds(org * part, part)

    def cost_copy(side):
        return pltpu.make_async_remote_copy(
            src_ref=costs.at[piece_of], dst_ref=raw.at[2 - side, piece_of], send_sem=cost_send.at[side, 0],
            recv_sem=cost_recv.at[side, 0], device_id={"blk": sides[side][1]}, device_id_type=MESH)

    def cost_spread(side, d):
        return pltpu.make_async_remote_copy(
            src_ref=raw.at[2 - side, piece_of], dst_ref=raw.at[2 - side, piece_of], send_sem=cost_send.at[side, d],
            recv_sem=cost_recv.at[side, d], device_id={"org": lax.rem(org + d, m)}, device_id_type=MESH)

    def source(side, j, h, start, count):
        row = jnp.where(side == 0, j - 1, rows - j)
        return warm.at[row, pl.ds(start, count), pl.ds(h * LANES, LANES)]

    def target(side, j, h, start, count):
        if isinstance(j, int) and j >= STEPS:
            return tail.at[1 - side, halves if j == HALO else h, pl.ds(start, count), :]
        row = jnp.where(side == 0, last + j, first - j)
        return grid.at[0, h, row, pl.ds(PAD + start, count), :]

    def unit(j, h):
        return last_unit if isinstance(j, int) and j == HALO else (j - 1) * halves + h

    def row_copy(side, j, h, count):
        u = unit(j, h)
        return pltpu.make_async_remote_copy(
            src_ref=source(side, j, h, 0, count), dst_ref=target(side, j, h, 0, count),
            send_sem=row_send.at[side, u, 0], recv_sem=row_recv.at[side, u, 0],
            device_id={"blk": jnp.where(side == 0, top, bottom)}, device_id_type=MESH)

    def to_relay(side, j, h):
        u = unit(j, h)
        return pltpu.make_async_remote_copy(
            src_ref=source(side, j, h, cut, cols - cut), dst_ref=relay.at[u],
            send_sem=row_send.at[side, u, 1], recv_sem=relay_in.at[u],
            device_id={"blk": via[side]}, device_id_type=MESH)

    def from_relay(side, j, h):
        u = unit(j, h)
        return pltpu.make_async_remote_copy(
            src_ref=relay.at[u], dst_ref=target(side, j, h, cut, cols - cut),
            send_sem=relay_out.at[u], recv_sem=row_recv.at[side, u, 1],
            device_id={"blk": goal[side]}, device_id_type=MESH)

    def each_send(j, h, side, act):
        there, split = sides[side][0], splits[side]
        @pl.when(there & jnp.logical_not(split) if relayed else there)
        def _():
            act(row_copy(side, j, h, cols))
        if relayed:
            @pl.when(split)
            def _():
                act(to_relay(side, j, h))
                act(row_copy(side, j, h, cut))

    def all_sends(act):
        def body(j, carry):
            for h in range(halves):
                for side in range(2):
                    each_send(j, h if side else halves - 1 - h, side, act)
            return carry
        lax.fori_loop(1, STEPS, body, 0)
        body(STEPS, 0)
        for side in range(2):
            each_send(HALO, 1 - side, side, act)

    def arrive(halo, j, h):
        side = 1 - halo
        there = jnp.where(halo == 0, has_top, has_bottom)
        split = jnp.where(halo == 0, me == goal[1], me == goal[0]) & there
        @pl.when(there & jnp.logical_not(split) if relayed else there)
        def _():
            pltpu.make_async_remote_copy(
                src_ref=source(0, 1, 0, 0, cols), dst_ref=target(side, j, h, 0, cols),
                send_sem=row_send.at[side, unit(j, h), 0], recv_sem=row_recv.at[side, unit(j, h), 0],
                device_id={"blk": bottom}, device_id_type=MESH).wait_recv()
        if relayed:
            @pl.when(split)
            def _():
                for part, start, count in ((0, 0, cut), (1, cut, cols - cut)):
                    pltpu.make_async_remote_copy(
                        src_ref=source(0, 1, 0, start, count), dst_ref=target(side, j, h, start, count),
                        send_sem=row_send.at[side, unit(j, h), part], recv_sem=row_recv.at[side, unit(j, h), part],
                        device_id={"blk": bottom}, device_id_type=MESH).wait_recv()

    def forward(j):
        if relayed:
            for side in range(2):
                @pl.when(me == via[side])
                def _():
                    for h in (1 - side, side)[:1 if isinstance(j, int) and j == HALO else 2]:
                        to_relay(side, j, h).wait_recv()
                        from_relay(side, j, h).start()

    for side in range(2):
        @pl.when(sides[side][0])
        def _():
            cost_copy(side).start()
    all_sends(lambda copy: copy.start())

    edge = jnp.full((PAD, LANES), far_value, jnp.float32)
    zero_edge = jnp.zeros((PAD, LANES), jnp.float32)

    def fill_edges(r, carry):
        for b in range(2):
            for h in range(halves):
                grid[b, h, r, pl.ds(0, PAD), :] = edge
                grid[b, h, r, pl.ds(PAD + cols, PAD), :] = edge
        return carry
    lax.fori_loop(0, total, fill_edges, 0)

    def fill_decay(r, carry):
        for h in range(halves):
            decay[h, r, pl.ds(0, PAD), :] = zero_edge
            decay[h, r, pl.ds(PAD + cols, PAD), :] = zero_edge
        return carry
    lax.fori_loop(0, rows + 2, fill_decay, 0)
    sums[...] = jnp.zeros_like(sums)
    raw[3] = jnp.zeros_like(raw[3])

    def fill_row(r):
        for h in range(halves):
            grid[0, h, r, inner, :] = jnp.full((cols, LANES), far_value, jnp.float32)
    for r in (0, 1, total - 2, total - 1):
        fill_row(r)
    for missing, block, begin in ((me == 0, 1, 2), (me == n - 1, 2, last + 1)):
        @pl.when(missing)
        def _():
            raw[block] = jnp.full(raw.shape[1:], far_value, jnp.float32)
            def fill(r, carry):
                fill_row(begin + r)
                return carry
            lax.fori_loop(0, STEPS - 1, fill, 0)

    def place(r):
        base = (me * rows + r - first) * cols
        names = [anchors[h] for h in range(halves)]
        for i in range(cols // CHUNK):
            node = lax.broadcasted_iota(jnp.int32, (CHUNK, LANES), 0) + (base + i * CHUNK)
            at = pl.ds(PAD + i * CHUNK, CHUNK)
            for h in range(halves):
                grid[0, h, r, at, :] = jnp.where(node == names[h], 0.0, grid[0, h, r, at, :])

    for side in range(2):
        @pl.when(sides[1 - side][0])
        def _():
            cost_copy(side).wait_recv()
            for d in range(1, m):
                cost_spread(side, d).start()

    for h in range(halves):
        own_rows(h).wait()

    def place_own(r, carry):
        place(r)
        return carry
    lax.fori_loop(first, last + 1, place_own, 0)

    own_cost.wait()
    for side in range(2):
        @pl.when(sides[1 - side][0])
        def _():
            for d in range(1, m):
                cost_spread(side, d).wait_recv()
    turned[...] = jnp.transpose(raw[...].reshape(4 * 4 * rows, cols))

    def widen(i, carry):
        at = pl.ds(pl.multiple_of(i * BAND, BAND), BAND)
        piece = turned[at, :]
        for r in range(1, total - 1):
            if r < first:
                block, row = 1, rows - first + r
            elif r <= last:
                block, row = 0, r - first
            else:
                block, row = 2, r - last - 1
            for k in range(4):
                lane = (block * 4 + k) * rows + row
                wide[k, r - 1, at, :] = jnp.broadcast_to(piece[:, lane:lane + 1], (BAND, LANES))
        return carry
    lax.fori_loop(0, cols // BAND, widen, 0)

    def best_of(old, r, i, hs):
        c0 = PAD + i * CHUNK
        at, mine = pl.ds(c0, CHUNK), pl.ds(i * CHUNK, CHUNK)
        price = [wide[k, r - 1, mine, :] for k in range(4)]
        result = []
        for h in hs:
            best = grid[old, h, r, at, :]
            best = jnp.minimum(best, grid[old, h, r, pl.ds(c0 - 1, CHUNK), :] + price[0])
            best = jnp.minimum(best, grid[old, h, r, pl.ds(c0 + 1, CHUNK), :] + price[1])
            best = jnp.minimum(best, grid[old, h, r - 1, at, :] + price[2])
            best = jnp.minimum(best, grid[old, h, r + 1, at, :] + price[3])
            result.append(best)
        return at, mine, result

    def relax(r, s, hs):
        old, new = lax.rem(s + 1, 2), lax.rem(s, 2)
        for i in range(cols // CHUNK):
            at, _, result = best_of(old, r, i, hs)
            for h, best in zip(hs, result):
                grid[new, h, r, at, :] = best

    both = tuple(range(halves))

    def finish(halo, j):
        r = jnp.where(halo == 0, first - j + STEPS, last + j - STEPS)
        q = r - first
        wants = [demand[h] for h in both]
        for i in range(cols // CHUNK):
            at, mine, result = best_of((STEPS + 1) % 2, r, i, both)
            for h, best in zip(both, result):
                final[q, mine, pl.ds(h * LANES, LANES)] = best
                power = best * RATE
                decay[h, q + 1, at, :] = jnp.exp2(-power)
                growth[h, q + 1, mine, :] = wants[h] * jnp.exp2(power)

    middle = rows // 2
    for s in range(1, middle):
        def inside(r, carry):
            relax(r, jnp.int32(s), both)
            return carry
        lax.fori_loop(first + s, last - s + 1, inside, 0)

    def stage(halo, j):
        for h in both:
            arrive(halo, j, h)
        place(jnp.where(halo == 0, first - j, last + j))

        def diagonal(s, carry):
            relax(jnp.where(halo == 0, first - j + s, last + j - s), s, both)
            return carry
        lax.fori_loop(1, jnp.minimum(STEPS - 1, j + middle - 1) + 1, diagonal, 0)

    def pair(q):
        return jnp.where(q == 0, early, late)

    def opening(j, carry):
        forward(j)

        def one(q, carry):
            stage(pair(q), j)
            return carry
        return lax.fori_loop(0, 2, one, carry)

    def closing(halo, j):
        stage(halo, j)
        finish(halo, j)

    ones = jnp.ones((8, 2 * LANES), jnp.bfloat16)

    def link(own, other, shift, hs, store):
        for c in range(0, cols, SPAN):
            term = None
            for h in hs:
                piece = growth[h, own, pl.ds(c, SPAN), :] * decay[h, other, pl.ds(PAD + c + shift, SPAN), :]
                term = piece if term is None else term + piece
            high = term.astype(jnp.bfloat16)
            low = (term - high.astype(jnp.float32)).astype(jnp.bfloat16)
            part = lax.dot_general(ones, jnp.concatenate([high, low], axis=1), (((1,), (1,)), ((), ())),
                                   preferred_element_type=jnp.float32)
            store(pl.ds(c, SPAN), part[0:1])

    def add_link(k, r, row, shift, hs):
        def store(at, part):
            sums[k, pl.ds(r - first, 1), at] = part
        link(r - first + 1, row - first + 1, shift, hs, store)

    def along(r, carry):
        add_link(0, r, r, -1, both)
        add_link(1, r, r, 1, both)
        return carry

    def across(r, carry):
        add_link(3, r, r + 1, 0, both)
        add_link(2, r + 1, r, 0, both)
        return carry

    def outer(halo):
        r0 = jnp.where(halo == 0, first - HALO, last + HALO)
        step = jnp.where(halo == 0, 1, -1)

        def diagonal(s, carry):
            relax(r0 + step * s, s, (halo,))
            return carry
        lax.fori_loop(1, STEPS + 1, diagonal, 0)

    scale = 1.0 / (m * halves * LANES)

    def cross(halo):
        there = jnp.where(halo == 0, has_top, has_bottom)
        r0 = jnp.where(halo == 0, first - HALO, last + HALO)
        step = jnp.where(halo == 0, 1, -1)
        own = jnp.where(halo == 0, 1, rows)
        other = jnp.where(halo == 0, 0, rows + 1)
        arrive(halo, HALO, halo)

        @pl.when(there)
        def _():
            base = (me * rows + r0 - first) * cols
            names, wants = anchors[halo], demand[halo]
            for i in range(cols // CHUNK):
                at, mine = pl.ds(PAD + i * CHUNK, CHUNK), pl.ds(i * CHUNK, CHUNK)
                node = lax.broadcasted_iota(jnp.int32, (CHUNK, LANES), 0) + (base + i * CHUNK)
                value = jnp.where(node == names, 0.0, tail[halo, halves, mine, :])
                for t in range(1, STEPS + 1):
                    value = value + wide[2 + halo, r0 + step * t - 1, mine, :]
                power = jnp.minimum(value, grid[STEPS % 2, halo, r0 + step * STEPS, at, :]) * RATE
                decay[halo, other, at, :] = jnp.exp2(-power)
                growth[halo, other, mine, :] = wants * jnp.exp2(power)

            def mine_store(at, part):
                sums[2 + halo, pl.ds(own - 1, 1), at] = part
            link(own, other, 0, (halo,), mine_store)

            def near_store(at, part):
                fee = raw[1 + halo, 3 - halo, pl.ds(jnp.where(halo == 0, rows - 1, 0), 1), at]
                value = part * jnp.exp(-temper * fee) * scale
                for c in range(0, at.size, width):
                    near_out[halo, (at.start + c) // width] = value[:, c:c + width]
            link(other, own, 0, (halo,), near_store)

    def near_copy(halo, p):
        return pltpu.make_async_remote_copy(
            src_ref=near_out.at[halo, p], dst_ref=near_in.at[1 - halo, org], send_sem=near_send.at[halo, p],
            recv_sem=near_recv.at[1 - halo, org], device_id={"blk": sides[halo][1], "org": p}, device_id_type=MESH)

    def near_wait(halo, p):
        pltpu.make_async_remote_copy(
            src_ref=near_out.at[halo, p], dst_ref=near_in.at[halo, p], send_sem=near_send.at[halo, p],
            recv_sem=near_recv.at[halo, p], device_id={"blk": sides[halo][1], "org": p}, device_id_type=MESH).wait_recv()

    def ahead(halo):
        def diagonal(s, carry):
            relax(jnp.where(halo == 0, first - STEPS + s, last + STEPS - s), s, both)
            return carry
        lax.fori_loop(1, STEPS + 1, diagonal, 0)

    def chain(halo, h):
        there = jnp.where(halo == 0, has_top, has_bottom)
        r0 = jnp.where(halo == 0, first - STEPS, last + STEPS)
        step = jnp.where(halo == 0, 1, -1)
        q = jnp.where(halo == 0, 0, rows - 1)
        arrive(halo, STEPS, h)

        @pl.when(there)
        def _():
            base = (me * rows + r0 - first) * cols
            for i in range(cols // CHUNK):
                at, mine = pl.ds(PAD + i * CHUNK, CHUNK), pl.ds(i * CHUNK, CHUNK)
                node = lax.broadcasted_iota(jnp.int32, (CHUNK, LANES), 0) + (base + i * CHUNK)
                value = jnp.where(node == anchors[h], 0.0, tail[halo, h, mine, :])
                grid[0, h, r0, at, :] = value
                for t in range(1, STEPS + 1):
                    r = r0 + step * t
                    value = jnp.minimum(grid[t % 2, h, r, at, :], value + wide[2 + halo, r - 1, mine, :])
                    grid[t % 2, h, r, at, :] = value

        def settle(h_static):
            for i in range(cols // CHUNK):
                at, mine = pl.ds(PAD + i * CHUNK, CHUNK), pl.ds(i * CHUNK, CHUNK)
                value = grid[STEPS % 2, h_static, q + first, at, :]
                final[q, mine, pl.ds(h_static * LANES, LANES)] = value
                power = value * RATE
                decay[h_static, q + 1, at, :] = jnp.exp2(-power)
                growth[h_static, q + 1, mine, :] = demand[h_static] * jnp.exp2(power)
        for k in both:
            @pl.when(h == k)
            def _():
                settle(k)

    bulk = STEPS // 2

    def closing_side(q, carry):
        halo = pair(q)

        def near(j, carry):
            @pl.when(q == 0)
            def _():
                forward(j)
            closing(halo, j)

            @pl.when(q == 1)
            def _():
                edge_links(j)
            return carry
        lax.fori_loop(bulk + 1, STEPS, near, 0)

        @pl.when(q == 0)
        def _():
            forward(STEPS)
            forward(HALO)
        ahead(halo)
        chain(halo, halo)
        outer(halo)
        chain(halo, 1 - halo)

        @pl.when(q == 0)
        def _():
            low = jnp.where(late == 0, first + bulk, first)
            lax.fori_loop(low, low + rows - bulk, along, 0)
            lax.fori_loop(low, low + rows - bulk - 1, across, 0)

        @pl.when(q == 1)
        def _():
            edge_links(STEPS)
        cross(halo)
        return carry

    def edge_links(j):
        r = jnp.where(late == 0, first - j + STEPS, last + j - STEPS)
        along(r, 0)
        across(r - late, 0)

    lax.fori_loop(1, bulk, opening, 0)
    forward(bulk)
    for q in range(2):
        closing(pair(q), bulk)
    lax.fori_loop(0, 2, closing_side, 0)

    ours = sums[...] * jnp.exp(-temper * raw[0]) * scale
    for p in range(m):
        share[p] = ours[:, :, p * width:(p + 1) * width]

    def org_copy(d):
        peer = lax.rem(org + d, m)
        return pltpu.make_async_remote_copy(
            src_ref=share.at[peer], dst_ref=landed.at[d - 1], send_sem=org_send.at[d - 1], recv_sem=org_recv.at[d - 1],
            device_id={"org": peer}, device_id_type=MESH)
    for halo in range(2):
        @pl.when(sides[halo][0])
        def _():
            for p in range(m):
                near_copy(halo, p).start()
    for d in range(1, m):
        org_copy(d).start()
    result = share[org]
    for d in range(1, m):
        org_copy(d).wait_recv()
        result += landed[d - 1]
    weights[...] = result
    for halo in range(2):
        @pl.when(sides[halo][0])
        def _():
            at = 0 if halo == 0 else rows - 1
            extra = weights[2 + halo, pl.ds(at, 1), :]
            for p in range(m):
                near_wait(halo, p)
                extra += near_in[halo, p]
            weights[2 + halo, pl.ds(at, 1), :] = extra

    for d in range(1, m):
        org_copy(d).wait_send()
    for side in range(2):
        @pl.when(sides[side][0])
        def _():
            cost_copy(side).wait_send()
            for p in range(m):
                near_copy(side, p).wait_send()
        @pl.when(sides[1 - side][0])
        def _():
            for d in range(1, m):
                cost_spread(side, d).wait_send()
    all_sends(lambda copy: copy.wait_send())
    if relayed:
        for side in range(2):
            @pl.when(me == via[side])
            def _():
                def body(j, carry):
                    for h in both:
                        from_relay(side, j, h).wait_send()
                    return carry
                lax.fori_loop(1, STEPS, body, 0)
                body(STEPS, 0)
                from_relay(side, HALO, 1 - side).wait_send()


def leave(rows, labels, weights, labels_out, weights_out, sems):
    copies = [pltpu.make_async_copy(labels.at[r], labels_out.at[r], sems.at[r]) for r in range(rows)]
    copies.append(pltpu.make_async_copy(weights, weights_out, sems.at[rows]))
    for copy in copies:
        copy.start()
    for copy in copies:
        copy.wait()


def local(n, m, warm_labels, link_costs, anchor_nodes, demand):
    rows, cols, count = warm_labels.shape
    halves = count // LANES
    total = rows + 2 * HALO
    width = cols // m
    units = STEPS * halves + 1
    any_space = pl.BlockSpec(memory_space=pl.ANY)
    vmem = pl.BlockSpec(memory_space=pltpu.VMEM)
    dma = pltpu.SemaphoreType.DMA
    labels, weights = pl.pallas_call(
        functools.partial(kernel, n, m, rows, cols, halves),
        out_shape=(
            pltpu.VMEM((rows, cols, count), jnp.float32),
            pltpu.VMEM((4, rows, width), jnp.float32),
        ),
        in_specs=[any_space, any_space, vmem, vmem],
        out_specs=(vmem, vmem),
        scratch_shapes=[
            pltpu.VMEM((2, halves, total, cols + 2 * PAD, LANES), jnp.float32),
            pltpu.VMEM((4, total - 2, cols, LANES), jnp.float32),
            pltpu.VMEM((4, 4, rows, cols), jnp.float32),
            pltpu.VMEM((cols, 16 * rows), jnp.float32),
            pltpu.VMEM((halves, rows + 2, cols + 2 * PAD, LANES), jnp.float32),
            pltpu.VMEM((halves, rows + 2, cols, LANES), jnp.float32),
            pltpu.VMEM((2, halves + 1, cols, LANES), jnp.float32),
            pltpu.VMEM((units, cols - cols // 2, LANES), jnp.float32),
            pltpu.VMEM((4, rows, cols), jnp.float32),
            pltpu.VMEM((m, 4, rows, width), jnp.float32),
            pltpu.VMEM((max(m - 1, 1), 4, rows, width), jnp.float32),
            pltpu.VMEM((2, m, 1, width), jnp.float32),
            pltpu.VMEM((2, m, 1, width), jnp.float32),
            dma((2, units, 2)),
            dma((2, units, 2)),
            dma((units,)),
            dma((units,)),
            dma((2, m)),
            dma((2, m)),
            dma((max(m - 1, 1),)),
            dma((max(m - 1, 1),)),
            dma((2, m)),
            dma((2, m)),
            dma((halves + 1,)),
        ],
        compiler_params=pltpu.CompilerParams(collective_id=0, has_side_effects=True, vmem_limit_bytes=58 * 1024 * 1024),
    )(warm_labels, link_costs, anchor_nodes.reshape(halves, 1, LANES), demand.reshape(halves, 1, LANES))
    labels = pltpu.with_memory_space_constraint(labels, pltpu.VMEM)
    weights = pltpu.with_memory_space_constraint(weights, pltpu.VMEM)
    return pl.pallas_call(
        functools.partial(leave, rows),
        out_shape=(
            jax.ShapeDtypeStruct((rows, cols, count), jnp.float32),
            jax.ShapeDtypeStruct((4, rows, width), jnp.float32),
        ),
        in_specs=[vmem, vmem],
        out_specs=(any_space, any_space),
        scratch_shapes=[dma((rows + 1,))],
        compiler_params=pltpu.CompilerParams(vmem_limit_bytes=8 * 1024 * 1024),
    )(labels, weights)


def solution(mesh):
    placed = (P("blk", None, "org"), P(None, "blk", None), P("org"), P("org"))
    return jax.shard_map(
        functools.partial(local, mesh.shape["blk"], mesh.shape["org"]),
        mesh=mesh,
        in_specs=placed,
        out_specs=(P("blk", None, "org"), P(None, "blk", "org")),
        check_vma=False,
    )
```

```python
import functools
import math

import jax
import jax.numpy as jnp
from jax import lax
from jax.experimental import pallas as pl
from jax.experimental.pallas import tpu as pltpu
from jax.sharding import PartitionSpec as P

INNER = 2
ROUNDS = 3
STEPS = INNER * ROUNDS
HALO = STEPS + 1

far_value = 1000000000.0
temper = 0.5
RATE = temper * math.log2(math.e)
LANES = 128
PAD = 8
CHUNK = 32
BAND = 64
SPAN = 256
MESH = pl.DeviceIdType.MESH


def kernel(n, m, rows, cols, halves, warm, costs, anchors, demand, final, weights, grid, wide, raw, turned, decay, growth, tail,
           relay, sums, share, landed, near_out, near_in, row_send, row_recv, relay_in, relay_out, cost_send, cost_recv,
           org_send, org_recv, near_send, near_recv, lend, lend_in, lend_out, lend_recv, ready, local_sem):
    me = lax.axis_index("blk")
    org = lax.axis_index("org")
    has_top = me > 0
    has_bottom = me < n - 1
    top = jnp.maximum(me - 1, 0)
    bottom = jnp.minimum(me + 1, n - 1)
    first, last = HALO, HALO + rows - 1
    total = rows + 2 * HALO
    inner = pl.ds(PAD, cols)
    sides = ((has_top, top), (has_bottom, bottom))
    mid = n // 2
    relayed = n == 8
    via = (0, n - 1)
    goal = (mid - 1, mid)
    splits = tuple(relayed and me == goal[1 - side] for side in range(2))
    cut = cols // 2
    width = cols // m
    late = lax.rem(me, 2)
    early = 1 - late
    last_unit = STEPS * halves
    plans = ((m - 1, 0, cols * 5 // 8), (m - 2, 1, cols * 3 // 16)) if relayed and m == 4 else ()
    paired = (me != 0) & (me != n - 1) & (me != mid - 1) & (me != mid)

    barrier = pltpu.get_barrier_semaphore()
    for there, who in sides:
        @pl.when(there)
        def _():
            pl.semaphore_signal(barrier, inc=1, device_id={"blk": who}, device_id_type=MESH)

    def greet(signal, p):
        pl.semaphore_signal(signal, inc=1, device_id={"org": p}, device_id_type=MESH)
        for there, who in sides:
            @pl.when(there)
            def _():
                pl.semaphore_signal(signal, inc=1, device_id={"blk": who, "org": p}, device_id_type=MESH)
    for p in range(1, m):
        @pl.when(org < p)
        def _():
            greet(barrier, p)
    if relayed:
        for a, b in ((mid - 1, 0), (mid - 1, n - 1), (mid, 0), (mid, n - 1)):
            for mine, other in ((a, b), (b, a)):
                @pl.when(me == mine)
                def _():
                    pl.semaphore_signal(barrier, inc=1, device_id={"blk": other}, device_id_type=MESH)
    own_cost = pltpu.make_async_copy(costs, raw.at[0], local_sem.at[halves])
    own_cost.start()

    def own_rows(h):
        return pltpu.make_async_copy(
            warm.at[:, :, pl.ds(h * LANES, LANES)],
            grid.at[0, h, pl.ds(first, rows), inner, :],
            local_sem.at[h])
    for h in range(halves):
        own_rows(h).start()
    around = jnp.where(has_top, 1, 0) + jnp.where(has_bottom, 1, 0)
    pl.semaphore_wait(barrier, around + org * (1 + around)
                      + (jnp.where((me == 0) | (me == n - 1) | (me == mid) | (me == mid - 1), 2, 0) if relayed else 0))

    part = 4 // m
    piece_of = pl.ds(org * part, part)

    def cost_copy(side):
        return pltpu.make_async_remote_copy(
            src_ref=costs.at[piece_of], dst_ref=raw.at[2 - side, piece_of], send_sem=cost_send.at[side, 0],
            recv_sem=cost_recv.at[side, 0], device_id={"blk": sides[side][1]}, device_id_type=MESH)

    def cost_spread(side, d):
        return pltpu.make_async_remote_copy(
            src_ref=raw.at[2 - side, piece_of], dst_ref=raw.at[2 - side, piece_of], send_sem=cost_send.at[side, d],
            recv_sem=cost_recv.at[side, d], device_id={"org": lax.rem(org + d, m)}, device_id_type=MESH)

    def source(side, j, h, start, count):
        row = jnp.where(side == 0, j - 1, rows - j)
        return warm.at[row, pl.ds(start, count), pl.ds(h * LANES, LANES)]

    def target(side, j, h, start, count):
        if isinstance(j, int) and j >= STEPS:
            return tail.at[1 - side, halves if j == HALO else h, pl.ds(start, count), :]
        row = jnp.where(side == 0, last + j, first - j)
        return grid.at[0, h, row, pl.ds(PAD + start, count), :]

    def unit(j, h):
        return last_unit if isinstance(j, int) and j == HALO else (j - 1) * halves + h

    def row_copy(side, j, h, count):
        u = unit(j, h)
        return pltpu.make_async_remote_copy(
            src_ref=source(side, j, h, 0, count), dst_ref=target(side, j, h, 0, count),
            send_sem=row_send.at[side, u, 0], recv_sem=row_recv.at[side, u, 0],
            device_id={"blk": jnp.where(side == 0, top, bottom)}, device_id_type=MESH)

    def to_relay(side, j, h):
        u = unit(j, h)
        return pltpu.make_async_remote_copy(
            src_ref=source(side, j, h, cut, cols - cut), dst_ref=relay.at[u],
            send_sem=row_send.at[side, u, 1], recv_sem=relay_in.at[u],
            device_id={"blk": via[side]}, device_id_type=MESH)

    def from_relay(side, j, h):
        u = unit(j, h)
        return pltpu.make_async_remote_copy(
            src_ref=relay.at[u], dst_ref=target(side, j, h, cut, cols - cut),
            send_sem=relay_out.at[u], recv_sem=row_recv.at[side, u, 1],
            device_id={"blk": goal[side]}, device_id_type=MESH)

    def each_send(j, h, side, act):
        there, split = sides[side][0], splits[side]
        @pl.when(there & jnp.logical_not(split) if relayed else there)
        def _():
            act(row_copy(side, j, h, cols))
        if relayed:
            @pl.when(split)
            def _():
                act(to_relay(side, j, h))
                act(row_copy(side, j, h, cut))

    def lend_copy(side, via_plane, moved):
        kept = cols - moved
        return pltpu.make_async_remote_copy(
            src_ref=source(side, HALO, 1 - side, kept, moved), dst_ref=lend.at[pl.ds(0, moved)],
            send_sem=row_send.at[side, last_unit, 1], recv_sem=lend_in.at[0],
            device_id={"blk": sides[side][1], "org": via_plane}, device_id_type=MESH)

    def lend_on(from_plane, moved):
        return pltpu.make_async_remote_copy(
            src_ref=lend.at[pl.ds(0, moved)], dst_ref=tail.at[late, halves, pl.ds(cols - moved, moved), :],
            send_sem=lend_out.at[0], recv_sem=lend_recv.at[0], device_id={"org": from_plane}, device_id_type=MESH)

    def outer_send(side, act):
        there, split = sides[side][0], splits[side]
        lending = paired & (late == side)
        plain = there
        for from_plane, via_plane, moved in plans:
            here = lending & (org == from_plane)
            plain = plain & jnp.logical_not(here)

            @pl.when(here)
            def _():
                act(row_copy(side, HALO, 1 - side, cols - moved))
                act(lend_copy(side, via_plane, moved))

        @pl.when(plain & jnp.logical_not(split) if relayed else plain)
        def _():
            act(row_copy(side, HALO, 1 - side, cols))
        if relayed:
            @pl.when(split)
            def _():
                act(to_relay(side, HALO, 1 - side))
                act(row_copy(side, HALO, 1 - side, cut))

    def all_sends(act):
        def body(j, carry):
            for h in range(halves):
                for side in range(2):
                    each_send(j, h if side else halves - 1 - h, side, act)
            return carry
        lax.fori_loop(1, STEPS, body, 0)
        body(STEPS, 0)
        for side in range(2):
            outer_send(side, act)

    def arrive(halo, j, h):
        side = 1 - halo
        there = jnp.where(halo == 0, has_top, has_bottom)
        split = jnp.where(halo == 0, me == goal[1], me == goal[0]) & there
        @pl.when(there & jnp.logical_not(split) if relayed else there)
        def _():
            pltpu.make_async_remote_copy(
                src_ref=source(0, 1, 0, 0, cols), dst_ref=target(side, j, h, 0, cols),
                send_sem=row_send.at[side, unit(j, h), 0], recv_sem=row_recv.at[side, unit(j, h), 0],
                device_id={"blk": bottom}, device_id_type=MESH).wait_recv()
        if relayed:
            @pl.when(split)
            def _():
                for part, start, count in ((0, 0, cut), (1, cut, cols - cut)):
                    pltpu.make_async_remote_copy(
                        src_ref=source(0, 1, 0, start, count), dst_ref=target(side, j, h, start, count),
                        send_sem=row_send.at[side, unit(j, h), part], recv_sem=row_recv.at[side, unit(j, h), part],
                        device_id={"blk": bottom}, device_id_type=MESH).wait_recv()

    def arrive_outer(halo):
        lending = paired & (late == halo)
        plain = jnp.bool_(True)
        for from_plane, _, moved in plans:
            here = lending & (org == from_plane)
            plain = plain & jnp.logical_not(here)

            @pl.when(here)
            def _():
                pltpu.make_async_remote_copy(
                    src_ref=source(0, 1, 0, 0, cols - moved), dst_ref=target(1 - halo, HALO, halo, 0, cols - moved),
                    send_sem=row_send.at[1 - halo, last_unit, 0], recv_sem=row_recv.at[1 - halo, last_unit, 0],
                    device_id={"blk": bottom}, device_id_type=MESH).wait_recv()
                lend_on(from_plane, moved).wait_recv()

        @pl.when(plain)
        def _():
            arrive(halo, HALO, halo)

    def forward(j):
        if relayed:
            for side in range(2):
                @pl.when(me == via[side])
                def _():
                    for h in (1 - side, side)[:1 if isinstance(j, int) and j == HALO else 2]:
                        to_relay(side, j, h).wait_recv()
                        from_relay(side, j, h).start()

    for side in range(2):
        @pl.when(sides[side][0])
        def _():
            cost_copy(side).start()
    all_sends(lambda copy: copy.start())
    for p in range(m - 1):
        @pl.when(org > p)
        def _():
            greet(ready, p)

    edge = jnp.full((PAD, LANES), far_value, jnp.float32)
    zero_edge = jnp.zeros((PAD, LANES), jnp.float32)

    def fill_edges(r, carry):
        for b in range(2):
            for h in range(halves):
                grid[b, h, r, pl.ds(0, PAD), :] = edge
                grid[b, h, r, pl.ds(PAD + cols, PAD), :] = edge
        return carry
    lax.fori_loop(0, total, fill_edges, 0)

    def fill_decay(r, carry):
        for h in range(halves):
            decay[h, r, pl.ds(0, PAD), :] = zero_edge
            decay[h, r, pl.ds(PAD + cols, PAD), :] = zero_edge
        return carry
    lax.fori_loop(0, rows + 2, fill_decay, 0)
    sums[...] = jnp.zeros_like(sums)
    raw[3] = jnp.zeros_like(raw[3])

    def fill_row(r):
        for h in range(halves):
            grid[0, h, r, inner, :] = jnp.full((cols, LANES), far_value, jnp.float32)
    for r in (0, 1, total - 2, total - 1):
        fill_row(r)
    for missing, block, begin in ((me == 0, 1, 2), (me == n - 1, 2, last + 1)):
        @pl.when(missing)
        def _():
            raw[block] = jnp.full(raw.shape[1:], far_value, jnp.float32)
            def fill(r, carry):
                fill_row(begin + r)
                return carry
            lax.fori_loop(0, STEPS - 1, fill, 0)

    def place(r):
        base = (me * rows + r - first) * cols
        names = [anchors[h] for h in range(halves)]
        for i in range(cols // CHUNK):
            node = lax.broadcasted_iota(jnp.int32, (CHUNK, LANES), 0) + (base + i * CHUNK)
            at = pl.ds(PAD + i * CHUNK, CHUNK)
            for h in range(halves):
                grid[0, h, r, at, :] = jnp.where(node == names[h], 0.0, grid[0, h, r, at, :])

    @pl.when(org < m - 1)
    def _():
        pl.semaphore_wait(ready, (m - 1 - org) * (1 + around))
    for side in range(2):
        @pl.when(sides[1 - side][0])
        def _():
            cost_copy(side).wait_recv()
            for d in range(1, m):
                cost_spread(side, d).start()

    for h in range(halves):
        own_rows(h).wait()

    def place_own(r, carry):
        place(r)
        return carry
    lax.fori_loop(first, last + 1, place_own, 0)

    own_cost.wait()
    for side in range(2):
        @pl.when(sides[1 - side][0])
        def _():
            for d in range(1, m):
                cost_spread(side, d).wait_recv()
    turned[...] = jnp.transpose(raw[...].reshape(4 * 4 * rows, cols))

    def widen(i, carry):
        at = pl.ds(pl.multiple_of(i * BAND, BAND), BAND)
        piece = turned[at, :]
        for r in range(1, total - 1):
            if r < first:
                block, row = 1, rows - first + r
            elif r <= last:
                block, row = 0, r - first
            else:
                block, row = 2, r - last - 1
            for k in range(4):
                lane = (block * 4 + k) * rows + row
                wide[k, r - 1, at, :] = jnp.broadcast_to(piece[:, lane:lane + 1], (BAND, LANES))
        return carry
    lax.fori_loop(0, cols // BAND, widen, 0)

    def best_of(old, r, i, hs):
        c0 = PAD + i * CHUNK
        at, mine = pl.ds(c0, CHUNK), pl.ds(i * CHUNK, CHUNK)
        price = [wide[k, r - 1, mine, :] for k in range(4)]
        result = []
        for h in hs:
            best = grid[old, h, r, at, :]
            best = jnp.minimum(best, grid[old, h, r, pl.ds(c0 - 1, CHUNK), :] + price[0])
            best = jnp.minimum(best, grid[old, h, r, pl.ds(c0 + 1, CHUNK), :] + price[1])
            best = jnp.minimum(best, grid[old, h, r - 1, at, :] + price[2])
            best = jnp.minimum(best, grid[old, h, r + 1, at, :] + price[3])
            result.append(best)
        return at, mine, result

    def relax(r, s, hs):
        old, new = lax.rem(s + 1, 2), lax.rem(s, 2)
        for i in range(cols // CHUNK):
            at, _, result = best_of(old, r, i, hs)
            for h, best in zip(hs, result):
                grid[new, h, r, at, :] = best

    both = tuple(range(halves))

    def finish(halo, j):
        r = jnp.where(halo == 0, first - j + STEPS, last + j - STEPS)
        q = r - first
        wants = [demand[h] for h in both]
        for i in range(cols // CHUNK):
            at, mine, result = best_of((STEPS + 1) % 2, r, i, both)
            for h, best in zip(both, result):
                final[q, mine, pl.ds(h * LANES, LANES)] = best
                power = best * RATE
                decay[h, q + 1, at, :] = jnp.exp2(-power)
                growth[h, q + 1, mine, :] = wants[h] * jnp.exp2(power)

    middle = rows // 2
    for s in range(1, middle):
        def inside(r, carry):
            relax(r, jnp.int32(s), both)
            return carry
        lax.fori_loop(first + s, last - s + 1, inside, 0)

    def stage(halo, j):
        for h in both:
            arrive(halo, j, h)
        place(jnp.where(halo == 0, first - j, last + j))

        def diagonal(s, carry):
            relax(jnp.where(halo == 0, first - j + s, last + j - s), s, both)
            return carry
        lax.fori_loop(1, jnp.minimum(STEPS - 1, j + middle - 1) + 1, diagonal, 0)

    def pair(q):
        return jnp.where(q == 0, early, late)

    def opening(j, carry):
        forward(j)

        def one(q, carry):
            stage(pair(q), j)
            return carry
        return lax.fori_loop(0, 2, one, carry)

    def closing(halo, j):
        stage(halo, j)
        finish(halo, j)

    ones = jnp.ones((8, 2 * LANES), jnp.bfloat16)

    def link(own, other, shift, hs, store):
        for c in range(0, cols, SPAN):
            term = None
            for h in hs:
                piece = growth[h, own, pl.ds(c, SPAN), :] * decay[h, other, pl.ds(PAD + c + shift, SPAN), :]
                term = piece if term is None else term + piece
            high = term.astype(jnp.bfloat16)
            low = (term - high.astype(jnp.float32)).astype(jnp.bfloat16)
            part = lax.dot_general(ones, jnp.concatenate([high, low], axis=1), (((1,), (1,)), ((), ())),
                                   preferred_element_type=jnp.float32)
            store(pl.ds(c, SPAN), part[0:1])

    def add_link(k, r, row, shift, hs):
        def store(at, part):
            sums[k, pl.ds(r - first, 1), at] = part
        link(r - first + 1, row - first + 1, shift, hs, store)

    def along(r, carry):
        add_link(0, r, r, -1, both)
        add_link(1, r, r, 1, both)
        return carry

    def across(r, carry):
        add_link(3, r, r + 1, 0, both)
        add_link(2, r + 1, r, 0, both)
        return carry

    def outer(halo):
        r0 = jnp.where(halo == 0, first - HALO, last + HALO)
        step = jnp.where(halo == 0, 1, -1)

        def diagonal(s, carry):
            relax(r0 + step * s, s, (halo,))
            return carry
        lax.fori_loop(1, STEPS + 1, diagonal, 0)

    scale = 1.0 / (m * halves * LANES)

    def cross(halo):
        there = jnp.where(halo == 0, has_top, has_bottom)
        r0 = jnp.where(halo == 0, first - HALO, last + HALO)
        step = jnp.where(halo == 0, 1, -1)
        own = jnp.where(halo == 0, 1, rows)
        other = jnp.where(halo == 0, 0, rows + 1)
        arrive_outer(halo)

        @pl.when(there)
        def _():
            base = (me * rows + r0 - first) * cols
            names, wants = anchors[halo], demand[halo]
            for i in range(cols // CHUNK):
                at, mine = pl.ds(PAD + i * CHUNK, CHUNK), pl.ds(i * CHUNK, CHUNK)
                node = lax.broadcasted_iota(jnp.int32, (CHUNK, LANES), 0) + (base + i * CHUNK)
                value = jnp.where(node == names, 0.0, tail[halo, halves, mine, :])
                for t in range(1, STEPS + 1):
                    value = value + wide[2 + halo, r0 + step * t - 1, mine, :]
                power = jnp.minimum(value, grid[STEPS % 2, halo, r0 + step * STEPS, at, :]) * RATE
                decay[halo, other, at, :] = jnp.exp2(-power)
                growth[halo, other, mine, :] = wants * jnp.exp2(power)

            def mine_store(at, part):
                sums[2 + halo, pl.ds(own - 1, 1), at] = part
            link(own, other, 0, (halo,), mine_store)

            def near_store(at, part):
                fee = raw[1 + halo, 3 - halo, pl.ds(jnp.where(halo == 0, rows - 1, 0), 1), at]
                value = part * jnp.exp(-temper * fee) * scale
                for c in range(0, at.size, width):
                    near_out[halo, (at.start + c) // width] = value[:, c:c + width]
            link(other, own, 0, (halo,), near_store)

    def near_copy(halo, p):
        return pltpu.make_async_remote_copy(
            src_ref=near_out.at[halo, p], dst_ref=near_in.at[1 - halo, org], send_sem=near_send.at[halo, p],
            recv_sem=near_recv.at[1 - halo, org], device_id={"blk": sides[halo][1], "org": p}, device_id_type=MESH)

    def near_wait(halo, p):
        pltpu.make_async_remote_copy(
            src_ref=near_out.at[halo, p], dst_ref=near_in.at[halo, p], send_sem=near_send.at[halo, p],
            recv_sem=near_recv.at[halo, p], device_id={"blk": sides[halo][1], "org": p}, device_id_type=MESH).wait_recv()

    def ahead(halo):
        def diagonal(s, carry):
            relax(jnp.where(halo == 0, first - STEPS + s, last + STEPS - s), s, both)
            return carry
        lax.fori_loop(1, STEPS + 1, diagonal, 0)

    def chain(halo, h):
        there = jnp.where(halo == 0, has_top, has_bottom)
        r0 = jnp.where(halo == 0, first - STEPS, last + STEPS)
        step = jnp.where(halo == 0, 1, -1)
        q = jnp.where(halo == 0, 0, rows - 1)
        arrive(halo, STEPS, h)

        @pl.when(there)
        def _():
            base = (me * rows + r0 - first) * cols
            for i in range(cols // CHUNK):
                at, mine = pl.ds(PAD + i * CHUNK, CHUNK), pl.ds(i * CHUNK, CHUNK)
                node = lax.broadcasted_iota(jnp.int32, (CHUNK, LANES), 0) + (base + i * CHUNK)
                value = jnp.where(node == anchors[h], 0.0, tail[halo, h, mine, :])
                grid[0, h, r0, at, :] = value
                for t in range(1, STEPS + 1):
                    r = r0 + step * t
                    value = jnp.minimum(grid[t % 2, h, r, at, :], value + wide[2 + halo, r - 1, mine, :])
                    grid[t % 2, h, r, at, :] = value

        def settle(h_static):
            for i in range(cols // CHUNK):
                at, mine = pl.ds(PAD + i * CHUNK, CHUNK), pl.ds(i * CHUNK, CHUNK)
                value = grid[STEPS % 2, h_static, q + first, at, :]
                final[q, mine, pl.ds(h_static * LANES, LANES)] = value
                power = value * RATE
                decay[h_static, q + 1, at, :] = jnp.exp2(-power)
                growth[h_static, q + 1, mine, :] = demand[h_static] * jnp.exp2(power)
        for k in both:
            @pl.when(h == k)
            def _():
                settle(k)

    bulk = STEPS // 2

    def closing_side(q, carry):
        halo = pair(q)

        def near(j, carry):
            @pl.when(q == 0)
            def _():
                forward(j)
            closing(halo, j)

            @pl.when(q == 1)
            def _():
                edge_links(j)
            return carry
        lax.fori_loop(bulk + 1, STEPS, near, 0)

        @pl.when(q == 0)
        def _():
            forward(STEPS)
            forward(HALO)
        ahead(halo)
        chain(halo, halo)
        outer(halo)
        chain(halo, 1 - halo)

        @pl.when(q == 0)
        def _():
            low = jnp.where(late == 0, first + bulk, first)
            lax.fori_loop(low, low + rows - bulk, along, 0)
            lax.fori_loop(low, low + rows - bulk - 1, across, 0)

        @pl.when(q == 1)
        def _():
            edge_links(STEPS)
        cross(halo)
        return carry

    def edge_links(j):
        r = jnp.where(late == 0, first - j + STEPS, last + j - STEPS)
        along(r, 0)
        across(r - late, 0)

    lax.fori_loop(1, bulk, opening, 0)
    for from_plane, via_plane, moved in plans:
        @pl.when(paired & (org == via_plane))
        def _():
            pltpu.make_async_remote_copy(
                src_ref=lend.at[pl.ds(0, moved)], dst_ref=lend.at[pl.ds(0, moved)], send_sem=lend_out.at[0],
                recv_sem=lend_in.at[0], device_id={"org": from_plane}, device_id_type=MESH).wait_recv()
            lend_on(from_plane, moved).start()
    forward(bulk)
    for q in range(2):
        closing(pair(q), bulk)
    lax.fori_loop(0, 2, closing_side, 0)

    ours = sums[...] * jnp.exp(-temper * raw[0]) * scale
    for p in range(m):
        share[p] = ours[:, :, p * width:(p + 1) * width]

    def org_copy(d):
        peer = lax.rem(org + d, m)
        return pltpu.make_async_remote_copy(
            src_ref=share.at[peer], dst_ref=landed.at[d - 1], send_sem=org_send.at[d - 1], recv_sem=org_recv.at[d - 1],
            device_id={"org": peer}, device_id_type=MESH)
    for halo in range(2):
        @pl.when(sides[halo][0])
        def _():
            for p in range(m):
                near_copy(halo, p).start()
    for d in range(1, m):
        org_copy(d).start()
    result = share[org]
    for d in range(1, m):
        org_copy(d).wait_recv()
        result += landed[d - 1]
    weights[...] = result
    for halo in range(2):
        @pl.when(sides[halo][0])
        def _():
            at = 0 if halo == 0 else rows - 1
            extra = weights[2 + halo, pl.ds(at, 1), :]
            for p in range(m):
                near_wait(halo, p)
                extra += near_in[halo, p]
            weights[2 + halo, pl.ds(at, 1), :] = extra

    for d in range(1, m):
        org_copy(d).wait_send()
    for side in range(2):
        @pl.when(sides[side][0])
        def _():
            cost_copy(side).wait_send()
            for p in range(m):
                near_copy(side, p).wait_send()
        @pl.when(sides[1 - side][0])
        def _():
            for d in range(1, m):
                cost_spread(side, d).wait_send()
    all_sends(lambda copy: copy.wait_send())
    for from_plane, via_plane, moved in plans:
        @pl.when(paired & (org == via_plane))
        def _():
            lend_on(from_plane, moved).wait_send()
    if relayed:
        for side in range(2):
            @pl.when(me == via[side])
            def _():
                def body(j, carry):
                    for h in both:
                        from_relay(side, j, h).wait_send()
                    return carry
                lax.fori_loop(1, STEPS, body, 0)
                body(STEPS, 0)
                from_relay(side, HALO, 1 - side).wait_send()


def leave(rows, labels, weights, labels_out, weights_out, sems):
    copies = [pltpu.make_async_copy(labels.at[r], labels_out.at[r], sems.at[r]) for r in range(rows)]
    copies.append(pltpu.make_async_copy(weights, weights_out, sems.at[rows]))
    for copy in copies:
        copy.start()
    for copy in copies:
        copy.wait()


def local(n, m, warm_labels, link_costs, anchor_nodes, demand):
    rows, cols, count = warm_labels.shape
    halves = count // LANES
    total = rows + 2 * HALO
    width = cols // m
    units = STEPS * halves + 1
    any_space = pl.BlockSpec(memory_space=pl.ANY)
    vmem = pl.BlockSpec(memory_space=pltpu.VMEM)
    dma = pltpu.SemaphoreType.DMA
    labels, weights = pl.pallas_call(
        functools.partial(kernel, n, m, rows, cols, halves),
        out_shape=(
            pltpu.VMEM((rows, cols, count), jnp.float32),
            pltpu.VMEM((4, rows, width), jnp.float32),
        ),
        in_specs=[any_space, any_space, vmem, vmem],
        out_specs=(vmem, vmem),
        scratch_shapes=[
            pltpu.VMEM((2, halves, total, cols + 2 * PAD, LANES), jnp.float32),
            pltpu.VMEM((4, total - 2, cols, LANES), jnp.float32),
            pltpu.VMEM((4, 4, rows, cols), jnp.float32),
            pltpu.VMEM((cols, 16 * rows), jnp.float32),
            pltpu.VMEM((halves, rows + 2, cols + 2 * PAD, LANES), jnp.float32),
            pltpu.VMEM((halves, rows + 2, cols, LANES), jnp.float32),
            pltpu.VMEM((2, halves + 1, cols, LANES), jnp.float32),
            pltpu.VMEM((units, cols - cols // 2, LANES), jnp.float32),
            pltpu.VMEM((4, rows, cols), jnp.float32),
            pltpu.VMEM((m, 4, rows, width), jnp.float32),
            pltpu.VMEM((max(m - 1, 1), 4, rows, width), jnp.float32),
            pltpu.VMEM((2, m, 1, width), jnp.float32),
            pltpu.VMEM((2, m, 1, width), jnp.float32),
            dma((2, units, 2)),
            dma((2, units, 2)),
            dma((units,)),
            dma((units,)),
            dma((2, m)),
            dma((2, m)),
            dma((max(m - 1, 1),)),
            dma((max(m - 1, 1),)),
            dma((2, m)),
            dma((2, m)),
            pltpu.VMEM((cols * 5 // 8, LANES), jnp.float32),
            dma((1,)),
            dma((1,)),
            dma((1,)),
            pltpu.SemaphoreType.REGULAR,
            dma((halves + 1,)),
        ],
        compiler_params=pltpu.CompilerParams(collective_id=0, has_side_effects=True, vmem_limit_bytes=58 * 1024 * 1024),
    )(warm_labels, link_costs, anchor_nodes.reshape(halves, 1, LANES), demand.reshape(halves, 1, LANES))
    labels = pltpu.with_memory_space_constraint(labels, pltpu.VMEM)
    weights = pltpu.with_memory_space_constraint(weights, pltpu.VMEM)
    return pl.pallas_call(
        functools.partial(leave, rows),
        out_shape=(
            jax.ShapeDtypeStruct((rows, cols, count), jnp.float32),
            jax.ShapeDtypeStruct((4, rows, width), jnp.float32),
        ),
        in_specs=[vmem, vmem],
        out_specs=(any_space, any_space),
        scratch_shapes=[dma((rows + 1,))],
        compiler_params=pltpu.CompilerParams(vmem_limit_bytes=8 * 1024 * 1024),
    )(labels, weights)


def solution(mesh):
    placed = (P("blk", None, "org"), P(None, "blk", None), P("org"), P("org"))
    return jax.shard_map(
        functools.partial(local, mesh.shape["blk"], mesh.shape["org"]),
        mesh=mesh,
        in_specs=placed,
        out_specs=(P("blk", None, "org"), P(None, "blk", "org")),
        check_vma=False,
    )
```

```python
import functools
import math

import jax
import jax.numpy as jnp
from jax import lax
from jax.experimental import pallas as pl
from jax.experimental.pallas import tpu as pltpu
from jax.sharding import PartitionSpec as P

INNER = 2
ROUNDS = 3
STEPS = INNER * ROUNDS
HALO = STEPS + 1

far_value = 1000000000.0
temper = 0.5
RATE = temper * math.log2(math.e)
LANES = 128
PAD = 8
CHUNK = 32
BAND = 64
SPAN = 256
MESH = pl.DeviceIdType.MESH


def kernel(n, m, rows, cols, halves, warm, costs, anchors_in, demand_in, final, weights, grid, wide, raw, turned, decay, growth, tail,
           relay, sums, share, landed, near_out, near_in, row_send, row_recv, relay_in, relay_out, cost_send, cost_recv,
           org_send, org_recv, near_send, near_recv, lend, lend_in, lend_out, lend_recv, ready, anchors, demand, fees, local_sem):
    me = lax.axis_index("blk")
    org = lax.axis_index("org")
    has_top = me > 0
    has_bottom = me < n - 1
    top = jnp.maximum(me - 1, 0)
    bottom = jnp.minimum(me + 1, n - 1)
    first, last = HALO, HALO + rows - 1
    total = rows + 2 * HALO
    inner = pl.ds(PAD, cols)
    sides = ((has_top, top), (has_bottom, bottom))
    mid = n // 2
    relayed = n == 8
    via = (0, n - 1)
    goal = (mid - 1, mid)
    splits = tuple(relayed and me == goal[1 - side] for side in range(2))
    cut = cols // 2
    width = cols // m
    late = lax.rem(me, 2)
    early = 1 - late
    last_unit = STEPS * halves
    plans = ((m - 1, 0, cols * 13 // 16), (m - 2, 1, cols * 9 // 32)) if relayed and m == 4 else ()
    paired = (me != 0) & (me != n - 1) & (me != mid - 1) & (me != mid)

    barrier = pltpu.get_barrier_semaphore()
    for there, who in sides:
        @pl.when(there)
        def _():
            pl.semaphore_signal(barrier, inc=1, device_id={"blk": who}, device_id_type=MESH)

    def greet(signal, p):
        pl.semaphore_signal(signal, inc=1, device_id={"org": p}, device_id_type=MESH)
        for there, who in sides:
            @pl.when(there)
            def _():
                pl.semaphore_signal(signal, inc=1, device_id={"blk": who, "org": p}, device_id_type=MESH)
    for p in range(1, m):
        @pl.when(org < p)
        def _():
            greet(barrier, p)
    if relayed:
        for a, b in ((mid - 1, 0), (mid - 1, n - 1), (mid, 0), (mid, n - 1)):
            for mine, other in ((a, b), (b, a)):
                @pl.when(me == mine)
                def _():
                    pl.semaphore_signal(barrier, inc=1, device_id={"blk": other}, device_id_type=MESH)
    own_cost = pltpu.make_async_copy(costs, raw.at[0], local_sem.at[halves])
    own_cost.start()
    listed = (pltpu.make_async_copy(anchors_in, anchors, local_sem.at[halves + 1]),
              pltpu.make_async_copy(demand_in, demand, local_sem.at[halves + 2]))
    for copy in listed:
        copy.start()

    def own_rows(h):
        return pltpu.make_async_copy(
            warm.at[:, :, pl.ds(h * LANES, LANES)],
            grid.at[0, h, pl.ds(first, rows), inner, :],
            local_sem.at[h])
    for h in range(halves):
        own_rows(h).start()
    around = jnp.where(has_top, 1, 0) + jnp.where(has_bottom, 1, 0)
    pl.semaphore_wait(barrier, around + org * (1 + around)
                      + (jnp.where((me == 0) | (me == n - 1) | (me == mid) | (me == mid - 1), 2, 0) if relayed else 0))

    part = 4 // m
    piece_of = pl.ds(org * part, part)

    def cost_copy(side):
        return pltpu.make_async_remote_copy(
            src_ref=costs.at[piece_of], dst_ref=raw.at[2 - side, piece_of], send_sem=cost_send.at[side, 0],
            recv_sem=cost_recv.at[side, 0], device_id={"blk": sides[side][1]}, device_id_type=MESH)

    def cost_spread(side, d):
        return pltpu.make_async_remote_copy(
            src_ref=raw.at[2 - side, piece_of], dst_ref=raw.at[2 - side, piece_of], send_sem=cost_send.at[side, d],
            recv_sem=cost_recv.at[side, d], device_id={"org": lax.rem(org + d, m)}, device_id_type=MESH)

    def source(side, j, h, start, count):
        row = jnp.where(side == 0, j - 1, rows - j)
        return warm.at[row, pl.ds(start, count), pl.ds(h * LANES, LANES)]

    def target(side, j, h, start, count):
        if isinstance(j, int) and j >= STEPS:
            return tail.at[1 - side, halves if j == HALO else h, pl.ds(start, count), :]
        row = jnp.where(side == 0, last + j, first - j)
        return grid.at[0, h, row, pl.ds(PAD + start, count), :]

    def unit(j, h):
        return last_unit if isinstance(j, int) and j == HALO else (j - 1) * halves + h

    def row_copy(side, j, h, count):
        u = unit(j, h)
        return pltpu.make_async_remote_copy(
            src_ref=source(side, j, h, 0, count), dst_ref=target(side, j, h, 0, count),
            send_sem=row_send.at[side, u, 0], recv_sem=row_recv.at[side, u, 0],
            device_id={"blk": jnp.where(side == 0, top, bottom)}, device_id_type=MESH)

    def to_relay(side, j, h):
        u = unit(j, h)
        return pltpu.make_async_remote_copy(
            src_ref=source(side, j, h, cut, cols - cut), dst_ref=relay.at[u],
            send_sem=row_send.at[side, u, 1], recv_sem=relay_in.at[u],
            device_id={"blk": via[side]}, device_id_type=MESH)

    def from_relay(side, j, h):
        u = unit(j, h)
        return pltpu.make_async_remote_copy(
            src_ref=relay.at[u], dst_ref=target(side, j, h, cut, cols - cut),
            send_sem=relay_out.at[u], recv_sem=row_recv.at[side, u, 1],
            device_id={"blk": goal[side]}, device_id_type=MESH)

    def each_send(j, h, side, act):
        there, split = sides[side][0], splits[side]
        @pl.when(there & jnp.logical_not(split) if relayed else there)
        def _():
            act(row_copy(side, j, h, cols))
        if relayed:
            @pl.when(split)
            def _():
                act(to_relay(side, j, h))
                act(row_copy(side, j, h, cut))

    def lend_copy(side, via_plane, moved):
        kept = cols - moved
        return pltpu.make_async_remote_copy(
            src_ref=source(side, HALO, 1 - side, kept, moved), dst_ref=lend.at[pl.ds(0, moved)],
            send_sem=row_send.at[side, last_unit, 1], recv_sem=lend_in.at[0],
            device_id={"blk": sides[side][1], "org": via_plane}, device_id_type=MESH)

    def lend_on(from_plane, moved):
        return pltpu.make_async_remote_copy(
            src_ref=lend.at[pl.ds(0, moved)], dst_ref=tail.at[late, halves, pl.ds(cols - moved, moved), :],
            send_sem=lend_out.at[0], recv_sem=lend_recv.at[0], device_id={"org": from_plane}, device_id_type=MESH)

    def outer_send(side, act):
        there, split = sides[side][0], splits[side]
        lending = paired & (late == side)
        plain = there
        for from_plane, via_plane, moved in plans:
            here = lending & (org == from_plane)
            plain = plain & jnp.logical_not(here)

            @pl.when(here)
            def _():
                act(row_copy(side, HALO, 1 - side, cols - moved))
                act(lend_copy(side, via_plane, moved))

        @pl.when(plain & jnp.logical_not(split) if relayed else plain)
        def _():
            act(row_copy(side, HALO, 1 - side, cols))
        if relayed:
            @pl.when(split)
            def _():
                act(to_relay(side, HALO, 1 - side))
                act(row_copy(side, HALO, 1 - side, cut))

    def all_sends(act):
        def body(j, carry):
            for h in range(halves):
                for side in range(2):
                    each_send(j, h if side else halves - 1 - h, side, act)
            return carry
        lax.fori_loop(1, STEPS, body, 0)
        body(STEPS, 0)
        for side in range(2):
            outer_send(side, act)

    def arrive(halo, j, h):
        side = 1 - halo
        there = jnp.where(halo == 0, has_top, has_bottom)
        split = jnp.where(halo == 0, me == goal[1], me == goal[0]) & there
        @pl.when(there & jnp.logical_not(split) if relayed else there)
        def _():
            pltpu.make_async_remote_copy(
                src_ref=source(0, 1, 0, 0, cols), dst_ref=target(side, j, h, 0, cols),
                send_sem=row_send.at[side, unit(j, h), 0], recv_sem=row_recv.at[side, unit(j, h), 0],
                device_id={"blk": bottom}, device_id_type=MESH).wait_recv()
        if relayed:
            @pl.when(split)
            def _():
                for part, start, count in ((0, 0, cut), (1, cut, cols - cut)):
                    pltpu.make_async_remote_copy(
                        src_ref=source(0, 1, 0, start, count), dst_ref=target(side, j, h, start, count),
                        send_sem=row_send.at[side, unit(j, h), part], recv_sem=row_recv.at[side, unit(j, h), part],
                        device_id={"blk": bottom}, device_id_type=MESH).wait_recv()

    def arrive_outer(halo):
        lending = paired & (late == halo)
        plain = jnp.bool_(True)
        for from_plane, _, moved in plans:
            here = lending & (org == from_plane)
            plain = plain & jnp.logical_not(here)

            @pl.when(here)
            def _():
                pltpu.make_async_remote_copy(
                    src_ref=source(0, 1, 0, 0, cols - moved), dst_ref=target(1 - halo, HALO, halo, 0, cols - moved),
                    send_sem=row_send.at[1 - halo, last_unit, 0], recv_sem=row_recv.at[1 - halo, last_unit, 0],
                    device_id={"blk": bottom}, device_id_type=MESH).wait_recv()
                lend_on(from_plane, moved).wait_recv()

        @pl.when(plain)
        def _():
            arrive(halo, HALO, halo)

    def forward(j):
        if relayed:
            for side in range(2):
                @pl.when(me == via[side])
                def _():
                    for h in (1 - side, side)[:1 if isinstance(j, int) and j == HALO else 2]:
                        to_relay(side, j, h).wait_recv()
                        from_relay(side, j, h).start()

    for side in range(2):
        @pl.when(sides[side][0])
        def _():
            cost_copy(side).start()
    all_sends(lambda copy: copy.start())
    for p in range(m - 1):
        @pl.when(org > p)
        def _():
            greet(ready, p)

    edge = jnp.full((PAD, LANES), far_value, jnp.float32)
    zero_edge = jnp.zeros((PAD, LANES), jnp.float32)

    def fill_edges(r, carry):
        for b in range(2):
            for h in range(halves):
                grid[b, h, r, pl.ds(0, PAD), :] = edge
                grid[b, h, r, pl.ds(PAD + cols, PAD), :] = edge
        return carry
    lax.fori_loop(0, total, fill_edges, 0)

    def fill_decay(r, carry):
        for h in range(halves):
            decay[h, r, pl.ds(0, PAD), :] = zero_edge
            decay[h, r, pl.ds(PAD + cols, PAD), :] = zero_edge
        return carry
    lax.fori_loop(0, rows + 2, fill_decay, 0)
    sums[...] = jnp.zeros_like(sums)
    raw[3] = jnp.zeros_like(raw[3])

    def fill_row(r):
        for h in range(halves):
            grid[0, h, r, inner, :] = jnp.full((cols, LANES), far_value, jnp.float32)
    for r in (0, 1, total - 2, total - 1):
        fill_row(r)
    for missing, block, begin in ((me == 0, 1, 2), (me == n - 1, 2, last + 1)):
        @pl.when(missing)
        def _():
            raw[block] = jnp.full(raw.shape[1:], far_value, jnp.float32)
            def fill(r, carry):
                fill_row(begin + r)
                return carry
            lax.fori_loop(0, STEPS - 1, fill, 0)

    def place(r):
        base = (me * rows + r - first) * cols
        names = [anchors[h] for h in range(halves)]
        for i in range(cols // CHUNK):
            node = lax.broadcasted_iota(jnp.int32, (CHUNK, LANES), 0) + (base + i * CHUNK)
            at = pl.ds(PAD + i * CHUNK, CHUNK)
            for h in range(halves):
                grid[0, h, r, at, :] = jnp.where(node == names[h], 0.0, grid[0, h, r, at, :])

    @pl.when(org < m - 1)
    def _():
        pl.semaphore_wait(ready, (m - 1 - org) * (1 + around))
    for side in range(2):
        @pl.when(sides[1 - side][0])
        def _():
            cost_copy(side).wait_recv()
            for d in range(1, m):
                cost_spread(side, d).start()

    for copy in listed:
        copy.wait()
    for h in range(halves):
        own_rows(h).wait()

    def place_own(r, carry):
        place(r)
        return carry
    lax.fori_loop(first, last + 1, place_own, 0)

    own_cost.wait()
    for side in range(2):
        @pl.when(sides[1 - side][0])
        def _():
            for d in range(1, m):
                cost_spread(side, d).wait_recv()
    turned[...] = jnp.transpose(raw[...].reshape(4 * 4 * rows, cols))

    def widen(i, carry):
        at = pl.ds(pl.multiple_of(i * BAND, BAND), BAND)
        piece = turned[at, :]
        for r in range(1, total - 1):
            if r < first:
                block, row = 1, rows - first + r
            elif r <= last:
                block, row = 0, r - first
            else:
                block, row = 2, r - last - 1
            for k in range(4):
                lane = (block * 4 + k) * rows + row
                wide[k, r - 1, at, :] = jnp.broadcast_to(piece[:, lane:lane + 1], (BAND, LANES))
        return carry
    lax.fori_loop(0, cols // BAND, widen, 0)

    def best_of(old, r, i, hs):
        c0 = PAD + i * CHUNK
        at, mine = pl.ds(c0, CHUNK), pl.ds(i * CHUNK, CHUNK)
        price = [wide[k, r - 1, mine, :] for k in range(4)]
        result = []
        for h in hs:
            best = grid[old, h, r, at, :]
            best = jnp.minimum(best, grid[old, h, r, pl.ds(c0 - 1, CHUNK), :] + price[0])
            best = jnp.minimum(best, grid[old, h, r, pl.ds(c0 + 1, CHUNK), :] + price[1])
            best = jnp.minimum(best, grid[old, h, r - 1, at, :] + price[2])
            best = jnp.minimum(best, grid[old, h, r + 1, at, :] + price[3])
            result.append(best)
        return at, mine, result

    def relax(r, s, hs):
        old, new = lax.rem(s + 1, 2), lax.rem(s, 2)
        for i in range(cols // CHUNK):
            at, _, result = best_of(old, r, i, hs)
            for h, best in zip(hs, result):
                grid[new, h, r, at, :] = best

    both = tuple(range(halves))

    def finish(halo, j):
        r = jnp.where(halo == 0, first - j + STEPS, last + j - STEPS)
        q = r - first
        wants = [demand[h] for h in both]
        for i in range(cols // CHUNK):
            at, mine, result = best_of((STEPS + 1) % 2, r, i, both)
            for h, best in zip(both, result):
                final[q, mine, pl.ds(h * LANES, LANES)] = best
                power = best * RATE
                decay[h, q + 1, at, :] = jnp.exp2(-power)
                growth[h, q + 1, mine, :] = wants[h] * jnp.exp2(power)

    middle = rows // 2
    for s in range(1, middle):
        def inside(r, carry):
            relax(r, jnp.int32(s), both)
            return carry
        lax.fori_loop(first + s, last - s + 1, inside, 0)

    def stage(halo, j):
        for h in both:
            arrive(halo, j, h)
        place(jnp.where(halo == 0, first - j, last + j))

        def diagonal(s, carry):
            relax(jnp.where(halo == 0, first - j + s, last + j - s), s, both)
            return carry
        lax.fori_loop(1, jnp.minimum(STEPS - 1, j + middle - 1) + 1, diagonal, 0)

    def pair(q):
        return jnp.where(q == 0, early, late)

    def opening(j, carry):
        forward(j)

        def one(q, carry):
            stage(pair(q), j)
            return carry
        return lax.fori_loop(0, 2, one, carry)

    def closing(halo, j):
        stage(halo, j)
        finish(halo, j)

    ones = jnp.ones((8, 2 * LANES), jnp.bfloat16)

    def link(own, other, shift, hs, store):
        for c in range(0, cols, SPAN):
            term = None
            for h in hs:
                piece = growth[h, own, pl.ds(c, SPAN), :] * decay[h, other, pl.ds(PAD + c + shift, SPAN), :]
                term = piece if term is None else term + piece
            high = term.astype(jnp.bfloat16)
            low = (term - high.astype(jnp.float32)).astype(jnp.bfloat16)
            part = lax.dot_general(ones, jnp.concatenate([high, low], axis=1), (((1,), (1,)), ((), ())),
                                   preferred_element_type=jnp.float32)
            store(pl.ds(c, SPAN), part[0:1])

    def add_link(k, r, row, shift, hs):
        def store(at, part):
            sums[k, pl.ds(r - first, 1), at] = part
        link(r - first + 1, row - first + 1, shift, hs, store)

    def along(r, carry):
        add_link(0, r, r, -1, both)
        add_link(1, r, r, 1, both)
        return carry

    def across(r, carry):
        add_link(3, r, r + 1, 0, both)
        add_link(2, r + 1, r, 0, both)
        return carry

    def outer(halo):
        r0 = jnp.where(halo == 0, first - HALO, last + HALO)
        step = jnp.where(halo == 0, 1, -1)

        def diagonal(s, carry):
            relax(r0 + step * s, s, (halo,))
            return carry
        lax.fori_loop(1, STEPS + 1, diagonal, 0)

    scale = 1.0 / (m * halves * LANES)

    def cross(halo):
        there = jnp.where(halo == 0, has_top, has_bottom)
        r0 = jnp.where(halo == 0, first - HALO, last + HALO)
        step = jnp.where(halo == 0, 1, -1)
        own = jnp.where(halo == 0, 1, rows)
        other = jnp.where(halo == 0, 0, rows + 1)
        arrive_outer(halo)

        @pl.when(there)
        def _():
            base = (me * rows + r0 - first) * cols
            names, wants = anchors[halo], demand[halo]
            for i in range(cols // CHUNK):
                at, mine = pl.ds(PAD + i * CHUNK, CHUNK), pl.ds(i * CHUNK, CHUNK)
                node = lax.broadcasted_iota(jnp.int32, (CHUNK, LANES), 0) + (base + i * CHUNK)
                value = jnp.where(node == names, 0.0, tail[halo, halves, mine, :])
                for t in range(1, STEPS + 1):
                    value = value + wide[2 + halo, r0 + step * t - 1, mine, :]
                power = jnp.minimum(value, grid[STEPS % 2, halo, r0 + step * STEPS, at, :]) * RATE
                decay[halo, other, at, :] = jnp.exp2(-power)
                growth[halo, other, mine, :] = wants * jnp.exp2(power)

            def mine_store(at, part):
                sums[2 + halo, pl.ds(own - 1, 1), at] = part
            link(own, other, 0, (halo,), mine_store)

            def near_store(at, part):
                value = part * fees[4 + halo, pl.ds(jnp.where(halo == 0, rows - 1, 0), 1), at]
                for c in range(0, at.size, width):
                    near_out[halo, (at.start + c) // width] = value[:, c:c + width]
            link(other, own, 0, (halo,), near_store)

    def near_copy(halo, p):
        return pltpu.make_async_remote_copy(
            src_ref=near_out.at[halo, p], dst_ref=near_in.at[1 - halo, org], send_sem=near_send.at[halo, p],
            recv_sem=near_recv.at[1 - halo, org], device_id={"blk": sides[halo][1], "org": p}, device_id_type=MESH)

    def near_wait(halo, p):
        pltpu.make_async_remote_copy(
            src_ref=near_out.at[halo, p], dst_ref=near_in.at[halo, p], send_sem=near_send.at[halo, p],
            recv_sem=near_recv.at[halo, p], device_id={"blk": sides[halo][1], "org": p}, device_id_type=MESH).wait_recv()

    def ahead(halo):
        def diagonal(s, carry):
            relax(jnp.where(halo == 0, first - STEPS + s, last + STEPS - s), s, both)
            return carry
        lax.fori_loop(1, STEPS + 1, diagonal, 0)

    def chain(halo, h):
        there = jnp.where(halo == 0, has_top, has_bottom)
        r0 = jnp.where(halo == 0, first - STEPS, last + STEPS)
        step = jnp.where(halo == 0, 1, -1)
        q = jnp.where(halo == 0, 0, rows - 1)
        arrive(halo, STEPS, h)

        @pl.when(there)
        def _():
            base = (me * rows + r0 - first) * cols
            for i in range(cols // CHUNK):
                at, mine = pl.ds(PAD + i * CHUNK, CHUNK), pl.ds(i * CHUNK, CHUNK)
                node = lax.broadcasted_iota(jnp.int32, (CHUNK, LANES), 0) + (base + i * CHUNK)
                value = jnp.where(node == anchors[h], 0.0, tail[halo, h, mine, :])
                grid[0, h, r0, at, :] = value
                for t in range(1, STEPS + 1):
                    r = r0 + step * t
                    value = jnp.minimum(grid[t % 2, h, r, at, :], value + wide[2 + halo, r - 1, mine, :])
                    grid[t % 2, h, r, at, :] = value

        def settle(h_static):
            for i in range(cols // CHUNK):
                at, mine = pl.ds(PAD + i * CHUNK, CHUNK), pl.ds(i * CHUNK, CHUNK)
                value = grid[STEPS % 2, h_static, q + first, at, :]
                final[q, mine, pl.ds(h_static * LANES, LANES)] = value
                power = value * RATE
                decay[h_static, q + 1, at, :] = jnp.exp2(-power)
                growth[h_static, q + 1, mine, :] = demand[h_static] * jnp.exp2(power)
        for k in both:
            @pl.when(h == k)
            def _():
                settle(k)

    bulk = STEPS // 2

    def closing_side(q, carry):
        halo = pair(q)

        def near(j, carry):
            @pl.when(q == 0)
            def _():
                forward(j)
            closing(halo, j)

            @pl.when(q == 1)
            def _():
                edge_links(j)
            return carry
        lax.fori_loop(bulk + 1, STEPS, near, 0)

        @pl.when(q == 0)
        def _():
            forward(STEPS)
            forward(HALO)
        ahead(halo)
        chain(halo, halo)
        outer(halo)
        chain(halo, 1 - halo)

        @pl.when(q == 0)
        def _():
            low = jnp.where(late == 0, first + bulk, first)
            lax.fori_loop(low, low + rows - bulk, along, 0)
            lax.fori_loop(low, low + rows - bulk - 1, across, 0)

        @pl.when(q == 1)
        def _():
            edge_links(STEPS)
        cross(halo)
        return carry

    def edge_links(j):
        r = jnp.where(late == 0, first - j + STEPS, last + j - STEPS)
        along(r, 0)
        across(r - late, 0)

    for k in range(4):
        fees[k] = jnp.exp(-temper * raw[0, k]) * scale
    for halo in range(2):
        fees[4 + halo] = jnp.exp(-temper * raw[1 + halo, 3 - halo]) * scale

    lax.fori_loop(1, bulk, opening, 0)
    for from_plane, via_plane, moved in plans:
        @pl.when(paired & (org == via_plane))
        def _():
            pltpu.make_async_remote_copy(
                src_ref=lend.at[pl.ds(0, moved)], dst_ref=lend.at[pl.ds(0, moved)], send_sem=lend_out.at[0],
                recv_sem=lend_in.at[0], device_id={"org": from_plane}, device_id_type=MESH).wait_recv()
            lend_on(from_plane, moved).start()
    forward(bulk)
    for q in range(2):
        closing(pair(q), bulk)
    lax.fori_loop(0, 2, closing_side, 0)

    for halo in range(2):
        @pl.when(sides[halo][0])
        def _():
            for p in range(m):
                near_copy(halo, p).start()
    for p in range(m):
        share[p] = sums[:, :, p * width:(p + 1) * width] * fees[0:4, :, p * width:(p + 1) * width]

    def org_copy(d):
        peer = lax.rem(org + d, m)
        return pltpu.make_async_remote_copy(
            src_ref=share.at[peer], dst_ref=landed.at[d - 1], send_sem=org_send.at[d - 1], recv_sem=org_recv.at[d - 1],
            device_id={"org": peer}, device_id_type=MESH)
    for d in range(1, m):
        org_copy(d).start()
    for side in range(2):
        @pl.when(sides[side][0])
        def _():
            cost_copy(side).wait_send()
        @pl.when(sides[1 - side][0])
        def _():
            for d in range(1, m):
                cost_spread(side, d).wait_send()
    all_sends(lambda copy: copy.wait_send())
    for from_plane, via_plane, moved in plans:
        @pl.when(paired & (org == via_plane))
        def _():
            lend_on(from_plane, moved).wait_send()
    if relayed:
        for side in range(2):
            @pl.when(me == via[side])
            def _():
                def body(j, carry):
                    for h in both:
                        from_relay(side, j, h).wait_send()
                    return carry
                lax.fori_loop(1, STEPS, body, 0)
                body(STEPS, 0)
                from_relay(side, HALO, 1 - side).wait_send()
    for d in range(1, m):
        org_copy(d).wait_send()
    for side in range(2):
        @pl.when(sides[side][0])
        def _():
            for p in range(m):
                near_copy(side, p).wait_send()
    result = share[org]
    for d in range(1, m):
        org_copy(d).wait_recv()
        result += landed[d - 1]
    weights[...] = result
    for halo in range(2):
        @pl.when(sides[halo][0])
        def _():
            at = 0 if halo == 0 else rows - 1
            extra = weights[2 + halo, pl.ds(at, 1), :]
            for p in range(m):
                near_wait(halo, p)
                extra += near_in[halo, p]
            weights[2 + halo, pl.ds(at, 1), :] = extra


def leave(rows, labels, weights, labels_out, weights_out, sems):
    copies = [pltpu.make_async_copy(labels.at[r], labels_out.at[r], sems.at[r]) for r in range(rows)]
    copies.append(pltpu.make_async_copy(weights, weights_out, sems.at[rows]))
    for copy in copies:
        copy.start()
    for copy in copies:
        copy.wait()


def local(n, m, warm_labels, link_costs, anchor_nodes, demand):
    rows, cols, count = warm_labels.shape
    halves = count // LANES
    total = rows + 2 * HALO
    width = cols // m
    units = STEPS * halves + 1
    any_space = pl.BlockSpec(memory_space=pl.ANY)
    vmem = pl.BlockSpec(memory_space=pltpu.VMEM)
    dma = pltpu.SemaphoreType.DMA
    labels, weights = pl.pallas_call(
        functools.partial(kernel, n, m, rows, cols, halves),
        out_shape=(
            pltpu.VMEM((rows, cols, count), jnp.float32),
            pltpu.VMEM((4, rows, width), jnp.float32),
        ),
        in_specs=[any_space] * 4,
        out_specs=(vmem, vmem),
        scratch_shapes=[
            pltpu.VMEM((2, halves, total, cols + 2 * PAD, LANES), jnp.float32),
            pltpu.VMEM((4, total - 2, cols, LANES), jnp.float32),
            pltpu.VMEM((4, 4, rows, cols), jnp.float32),
            pltpu.VMEM((cols, 16 * rows), jnp.float32),
            pltpu.VMEM((halves, rows + 2, cols + 2 * PAD, LANES), jnp.float32),
            pltpu.VMEM((halves, rows + 2, cols, LANES), jnp.float32),
            pltpu.VMEM((2, halves + 1, cols, LANES), jnp.float32),
            pltpu.VMEM((units, cols - cols // 2, LANES), jnp.float32),
            pltpu.VMEM((4, rows, cols), jnp.float32),
            pltpu.VMEM((m, 4, rows, width), jnp.float32),
            pltpu.VMEM((max(m - 1, 1), 4, rows, width), jnp.float32),
            pltpu.VMEM((2, m, 1, width), jnp.float32),
            pltpu.VMEM((2, m, 1, width), jnp.float32),
            dma((2, units, 2)),
            dma((2, units, 2)),
            dma((units,)),
            dma((units,)),
            dma((2, m)),
            dma((2, m)),
            dma((max(m - 1, 1),)),
            dma((max(m - 1, 1),)),
            dma((2, m)),
            dma((2, m)),
            pltpu.VMEM((cols * 13 // 16, LANES), jnp.float32),
            dma((1,)),
            dma((1,)),
            dma((1,)),
            pltpu.SemaphoreType.REGULAR,
            pltpu.VMEM((halves, 1, LANES), jnp.int32),
            pltpu.VMEM((halves, 1, LANES), jnp.float32),
            pltpu.VMEM((6, rows, cols), jnp.float32),
            dma((halves + 3,)),
        ],
        compiler_params=pltpu.CompilerParams(collective_id=0, has_side_effects=True, vmem_limit_bytes=58 * 1024 * 1024),
    )(warm_labels, link_costs, anchor_nodes.reshape(halves, 1, LANES), demand.reshape(halves, 1, LANES))
    labels = pltpu.with_memory_space_constraint(labels, pltpu.VMEM)
    weights = pltpu.with_memory_space_constraint(weights, pltpu.VMEM)
    return pl.pallas_call(
        functools.partial(leave, rows),
        out_shape=(
            jax.ShapeDtypeStruct((rows, cols, count), jnp.float32),
            jax.ShapeDtypeStruct((4, rows, width), jnp.float32),
        ),
        in_specs=[vmem, vmem],
        out_specs=(any_space, any_space),
        scratch_shapes=[dma((rows + 1,))],
        compiler_params=pltpu.CompilerParams(vmem_limit_bytes=8 * 1024 * 1024),
    )(labels, weights)


def solution(mesh):
    placed = (P("blk", None, "org"), P(None, "blk", None), P("org"), P("org"))
    return jax.shard_map(
        functools.partial(local, mesh.shape["blk"], mesh.shape["org"]),
        mesh=mesh,
        in_specs=placed,
        out_specs=(P("blk", None, "org"), P(None, "blk", "org")),
        check_vma=False,
    )
```

```python
import functools
import math

import jax
import jax.numpy as jnp
from jax import lax
from jax.experimental import pallas as pl
from jax.experimental.pallas import tpu as pltpu
from jax.sharding import PartitionSpec as P

INNER = 2
ROUNDS = 3
STEPS = INNER * ROUNDS
HALO = STEPS + 1

far_value = 1000000000.0
temper = 0.5
RATE = temper * math.log2(math.e)
LANES = 128
PAD = 8
CHUNK = 32
BAND = 64
SPAN = 256
MESH = pl.DeviceIdType.MESH


def kernel(n, m, rows, cols, halves, warm, costs, anchors_in, demand_in, final, weights, grid, wide, raw, turned, decay, growth, tail,
           relay, sums, share, landed, near_out, near_in, row_send, row_recv, relay_in, relay_out, cost_send, cost_recv,
           org_send, org_recv, near_send, near_recv, lend, lend_in, lend_out, lend_recv, ready, anchors, demand, fees, local_sem):
    me = lax.axis_index("blk")
    org = lax.axis_index("org")
    has_top = me > 0
    has_bottom = me < n - 1
    top = jnp.maximum(me - 1, 0)
    bottom = jnp.minimum(me + 1, n - 1)
    first, last = HALO, HALO + rows - 1
    total = rows + 2 * HALO
    inner = pl.ds(PAD, cols)
    sides = ((has_top, top), (has_bottom, bottom))
    mid = n // 2
    relayed = n == 8
    via = (0, n - 1)
    goal = (mid - 1, mid)
    splits = tuple(relayed and me == goal[1 - side] for side in range(2))
    cut = cols // 2
    width = cols // m
    late = lax.rem(me, 2)
    early = 1 - late
    last_unit = STEPS * halves
    plans = ((m - 1, 0, cols * 13 // 16), (m - 2, 1, cols * 9 // 32)) if relayed and m == 4 else ()
    paired = (me != 0) & (me != n - 1) & (me != mid - 1) & (me != mid)

    barrier = pltpu.get_barrier_semaphore()
    for there, who in sides:
        @pl.when(there)
        def _():
            pl.semaphore_signal(barrier, inc=1, device_id={"blk": who}, device_id_type=MESH)

    def greet(signal, p):
        pl.semaphore_signal(signal, inc=1, device_id={"org": p}, device_id_type=MESH)
        for there, who in sides:
            @pl.when(there)
            def _():
                pl.semaphore_signal(signal, inc=1, device_id={"blk": who, "org": p}, device_id_type=MESH)
    for p in range(1, m):
        @pl.when(org < p)
        def _():
            greet(barrier, p)
    if relayed:
        for a, b in ((mid - 1, 0), (mid - 1, n - 1), (mid, 0), (mid, n - 1)):
            for mine, other in ((a, b), (b, a)):
                @pl.when(me == mine)
                def _():
                    pl.semaphore_signal(barrier, inc=1, device_id={"blk": other}, device_id_type=MESH)
    own_cost = pltpu.make_async_copy(costs, raw.at[0], local_sem.at[halves])
    own_cost.start()
    listed = (pltpu.make_async_copy(anchors_in, anchors, local_sem.at[halves + 1]),
              pltpu.make_async_copy(demand_in, demand, local_sem.at[halves + 2]))
    for copy in listed:
        copy.start()

    def own_rows(h):
        return pltpu.make_async_copy(
            warm.at[:, :, pl.ds(h * LANES, LANES)],
            grid.at[0, h, pl.ds(first, rows), inner, :],
            local_sem.at[h])
    for h in range(halves):
        own_rows(h).start()
    around = jnp.where(has_top, 1, 0) + jnp.where(has_bottom, 1, 0)
    pl.semaphore_wait(barrier, around + org * (1 + around)
                      + (jnp.where((me == 0) | (me == n - 1) | (me == mid) | (me == mid - 1), 2, 0) if relayed else 0))

    part = 4 // m
    piece_of = pl.ds(org * part, part)

    def cost_copy(side):
        return pltpu.make_async_remote_copy(
            src_ref=costs.at[piece_of], dst_ref=raw.at[2 - side, piece_of], send_sem=cost_send.at[side, 0],
            recv_sem=cost_recv.at[side, 0], device_id={"blk": sides[side][1]}, device_id_type=MESH)

    def cost_spread(side, d):
        return pltpu.make_async_remote_copy(
            src_ref=raw.at[2 - side, piece_of], dst_ref=raw.at[2 - side, piece_of], send_sem=cost_send.at[side, d],
            recv_sem=cost_recv.at[side, d], device_id={"org": lax.rem(org + d, m)}, device_id_type=MESH)

    def source(side, j, h, start, count):
        row = jnp.where(side == 0, j - 1, rows - j)
        return warm.at[row, pl.ds(start, count), pl.ds(h * LANES, LANES)]

    def target(side, j, h, start, count):
        if isinstance(j, int) and j >= STEPS:
            return tail.at[1 - side, halves if j == HALO else h, pl.ds(start, count), :]
        row = jnp.where(side == 0, last + j, first - j)
        return grid.at[0, h, row, pl.ds(PAD + start, count), :]

    def unit(j, h):
        return last_unit if isinstance(j, int) and j == HALO else (j - 1) * halves + h

    def row_copy(side, j, h, count):
        u = unit(j, h)
        return pltpu.make_async_remote_copy(
            src_ref=source(side, j, h, 0, count), dst_ref=target(side, j, h, 0, count),
            send_sem=row_send.at[side, u, 0], recv_sem=row_recv.at[side, u, 0],
            device_id={"blk": jnp.where(side == 0, top, bottom)}, device_id_type=MESH)

    def to_relay(side, j, h):
        u = unit(j, h)
        return pltpu.make_async_remote_copy(
            src_ref=source(side, j, h, cut, cols - cut), dst_ref=relay.at[u],
            send_sem=row_send.at[side, u, 1], recv_sem=relay_in.at[u],
            device_id={"blk": via[side]}, device_id_type=MESH)

    def from_relay(side, j, h):
        u = unit(j, h)
        return pltpu.make_async_remote_copy(
            src_ref=relay.at[u], dst_ref=target(side, j, h, cut, cols - cut),
            send_sem=relay_out.at[u], recv_sem=row_recv.at[side, u, 1],
            device_id={"blk": goal[side]}, device_id_type=MESH)

    def each_send(j, h, side, act):
        there, split = sides[side][0], splits[side]
        @pl.when(there & jnp.logical_not(split) if relayed else there)
        def _():
            act(row_copy(side, j, h, cols))
        if relayed:
            @pl.when(split)
            def _():
                act(to_relay(side, j, h))
                act(row_copy(side, j, h, cut))

    def lend_copy(side, via_plane, moved):
        kept = cols - moved
        return pltpu.make_async_remote_copy(
            src_ref=source(side, HALO, 1 - side, kept, moved), dst_ref=lend.at[pl.ds(0, moved)],
            send_sem=row_send.at[side, last_unit, 1], recv_sem=lend_in.at[0],
            device_id={"blk": sides[side][1], "org": via_plane}, device_id_type=MESH)

    def lend_on(from_plane, moved):
        return pltpu.make_async_remote_copy(
            src_ref=lend.at[pl.ds(0, moved)], dst_ref=tail.at[late, halves, pl.ds(cols - moved, moved), :],
            send_sem=lend_out.at[0], recv_sem=lend_recv.at[0], device_id={"org": from_plane}, device_id_type=MESH)

    def outer_send(side, act):
        there, split = sides[side][0], splits[side]
        lending = paired & (late == side)
        plain = there
        for from_plane, via_plane, moved in plans:
            here = lending & (org == from_plane)
            plain = plain & jnp.logical_not(here)

            @pl.when(here)
            def _():
                act(row_copy(side, HALO, 1 - side, cols - moved))
                act(lend_copy(side, via_plane, moved))

        @pl.when(plain & jnp.logical_not(split) if relayed else plain)
        def _():
            act(row_copy(side, HALO, 1 - side, cols))
        if relayed:
            @pl.when(split)
            def _():
                act(to_relay(side, HALO, 1 - side))
                act(row_copy(side, HALO, 1 - side, cut))

    def all_sends(act):
        def body(j, carry):
            for h in range(halves):
                for side in range(2):
                    each_send(j, h if side else halves - 1 - h, side, act)
            return carry
        lax.fori_loop(1, STEPS, body, 0)
        for side in range(2):
            each_send(STEPS, 1 - side, side, act)
        for side in range(2):
            outer_send(side, act)
        for side in range(2):
            each_send(STEPS, side, side, act)

    def arrive(halo, j, h):
        side = 1 - halo
        there = jnp.where(halo == 0, has_top, has_bottom)
        split = jnp.where(halo == 0, me == goal[1], me == goal[0]) & there
        @pl.when(there & jnp.logical_not(split) if relayed else there)
        def _():
            pltpu.make_async_remote_copy(
                src_ref=source(0, 1, 0, 0, cols), dst_ref=target(side, j, h, 0, cols),
                send_sem=row_send.at[side, unit(j, h), 0], recv_sem=row_recv.at[side, unit(j, h), 0],
                device_id={"blk": bottom}, device_id_type=MESH).wait_recv()
        if relayed:
            @pl.when(split)
            def _():
                for part, start, count in ((0, 0, cut), (1, cut, cols - cut)):
                    pltpu.make_async_remote_copy(
                        src_ref=source(0, 1, 0, start, count), dst_ref=target(side, j, h, start, count),
                        send_sem=row_send.at[side, unit(j, h), part], recv_sem=row_recv.at[side, unit(j, h), part],
                        device_id={"blk": bottom}, device_id_type=MESH).wait_recv()

    def arrive_outer(halo):
        lending = paired & (late == halo)
        plain = jnp.bool_(True)
        for from_plane, _, moved in plans:
            here = lending & (org == from_plane)
            plain = plain & jnp.logical_not(here)

            @pl.when(here)
            def _():
                pltpu.make_async_remote_copy(
                    src_ref=source(0, 1, 0, 0, cols - moved), dst_ref=target(1 - halo, HALO, halo, 0, cols - moved),
                    send_sem=row_send.at[1 - halo, last_unit, 0], recv_sem=row_recv.at[1 - halo, last_unit, 0],
                    device_id={"blk": bottom}, device_id_type=MESH).wait_recv()
                lend_on(from_plane, moved).wait_recv()

        @pl.when(plain)
        def _():
            arrive(halo, HALO, halo)

    def forward(j):
        if relayed:
            for side in range(2):
                @pl.when(me == via[side])
                def _():
                    for h in (1 - side, side)[:1 if isinstance(j, int) and j == HALO else 2]:
                        to_relay(side, j, h).wait_recv()
                        from_relay(side, j, h).start()

    for side in range(2):
        @pl.when(sides[side][0])
        def _():
            cost_copy(side).start()
    all_sends(lambda copy: copy.start())
    for p in range(m - 1):
        @pl.when(org > p)
        def _():
            greet(ready, p)

    edge = jnp.full((PAD, LANES), far_value, jnp.float32)
    zero_edge = jnp.zeros((PAD, LANES), jnp.float32)

    def fill_edges(r, carry):
        for b in range(2):
            for h in range(halves):
                grid[b, h, r, pl.ds(0, PAD), :] = edge
                grid[b, h, r, pl.ds(PAD + cols, PAD), :] = edge
        return carry
    lax.fori_loop(0, total, fill_edges, 0)

    def fill_decay(r, carry):
        for h in range(halves):
            decay[h, r, pl.ds(0, PAD), :] = zero_edge
            decay[h, r, pl.ds(PAD + cols, PAD), :] = zero_edge
        return carry
    lax.fori_loop(0, rows + 2, fill_decay, 0)
    sums[...] = jnp.zeros_like(sums)
    raw[3] = jnp.zeros_like(raw[3])

    def fill_row(r):
        for h in range(halves):
            grid[0, h, r, inner, :] = jnp.full((cols, LANES), far_value, jnp.float32)
    for r in (0, 1, total - 2, total - 1):
        fill_row(r)
    for missing, block, begin in ((me == 0, 1, 2), (me == n - 1, 2, last + 1)):
        @pl.when(missing)
        def _():
            raw[block] = jnp.full(raw.shape[1:], far_value, jnp.float32)
            def fill(r, carry):
                fill_row(begin + r)
                return carry
            lax.fori_loop(0, STEPS - 1, fill, 0)

    def place(r):
        base = (me * rows + r - first) * cols
        names = [anchors[h] for h in range(halves)]
        for i in range(cols // CHUNK):
            node = lax.broadcasted_iota(jnp.int32, (CHUNK, LANES), 0) + (base + i * CHUNK)
            at = pl.ds(PAD + i * CHUNK, CHUNK)
            for h in range(halves):
                grid[0, h, r, at, :] = jnp.where(node == names[h], 0.0, grid[0, h, r, at, :])

    @pl.when(org < m - 1)
    def _():
        pl.semaphore_wait(ready, (m - 1 - org) * (1 + around))
    for side in range(2):
        @pl.when(sides[1 - side][0])
        def _():
            cost_copy(side).wait_recv()
            for d in range(1, m):
                cost_spread(side, d).start()

    for copy in listed:
        copy.wait()
    for h in range(halves):
        own_rows(h).wait()

    def place_own(r, carry):
        place(r)
        return carry
    lax.fori_loop(first, last + 1, place_own, 0)

    own_cost.wait()
    for side in range(2):
        @pl.when(sides[1 - side][0])
        def _():
            for d in range(1, m):
                cost_spread(side, d).wait_recv()
    turned[...] = jnp.transpose(raw[...].reshape(4 * 4 * rows, cols))

    def widen(i, carry):
        at = pl.ds(pl.multiple_of(i * BAND, BAND), BAND)
        piece = turned[at, :]
        for r in range(1, total - 1):
            if r < first:
                block, row = 1, rows - first + r
            elif r <= last:
                block, row = 0, r - first
            else:
                block, row = 2, r - last - 1
            for k in range(4):
                lane = (block * 4 + k) * rows + row
                wide[k, r - 1, at, :] = jnp.broadcast_to(piece[:, lane:lane + 1], (BAND, LANES))
        return carry
    lax.fori_loop(0, cols // BAND, widen, 0)

    def best_of(old, r, i, hs):
        c0 = PAD + i * CHUNK
        at, mine = pl.ds(c0, CHUNK), pl.ds(i * CHUNK, CHUNK)
        price = [wide[k, r - 1, mine, :] for k in range(4)]
        result = []
        for h in hs:
            best = grid[old, h, r, at, :]
            best = jnp.minimum(best, grid[old, h, r, pl.ds(c0 - 1, CHUNK), :] + price[0])
            best = jnp.minimum(best, grid[old, h, r, pl.ds(c0 + 1, CHUNK), :] + price[1])
            best = jnp.minimum(best, grid[old, h, r - 1, at, :] + price[2])
            best = jnp.minimum(best, grid[old, h, r + 1, at, :] + price[3])
            result.append(best)
        return at, mine, result

    def relax(r, s, hs):
        old, new = lax.rem(s + 1, 2), lax.rem(s, 2)
        for i in range(cols // CHUNK):
            at, _, result = best_of(old, r, i, hs)
            for h, best in zip(hs, result):
                grid[new, h, r, at, :] = best

    both = tuple(range(halves))

    def finish(halo, j):
        r = jnp.where(halo == 0, first - j + STEPS, last + j - STEPS)
        q = r - first
        wants = [demand[h] for h in both]
        for i in range(cols // CHUNK):
            at, mine, result = best_of((STEPS + 1) % 2, r, i, both)
            for h, best in zip(both, result):
                final[q, mine, pl.ds(h * LANES, LANES)] = best
                power = best * RATE
                decay[h, q + 1, at, :] = jnp.exp2(-power)
                growth[h, q + 1, mine, :] = wants[h] * jnp.exp2(power)

    middle = rows // 2
    for s in range(1, middle):
        def inside(r, carry):
            relax(r, jnp.int32(s), both)
            return carry
        lax.fori_loop(first + s, last - s + 1, inside, 0)

    def stage(halo, j):
        for h in both:
            arrive(halo, j, h)
        place(jnp.where(halo == 0, first - j, last + j))

        def diagonal(s, carry):
            relax(jnp.where(halo == 0, first - j + s, last + j - s), s, both)
            return carry
        lax.fori_loop(1, jnp.minimum(STEPS - 1, j + middle - 1) + 1, diagonal, 0)

    def pair(q):
        return jnp.where(q == 0, early, late)

    def opening(j, carry):
        forward(j)

        def one(q, carry):
            stage(pair(q), j)
            return carry
        return lax.fori_loop(0, 2, one, carry)

    def closing(halo, j):
        stage(halo, j)
        finish(halo, j)

    ones = jnp.ones((8, 2 * LANES), jnp.bfloat16)

    def link(own, other, shift, hs, store):
        for c in range(0, cols, SPAN):
            term = None
            for h in hs:
                piece = growth[h, own, pl.ds(c, SPAN), :] * decay[h, other, pl.ds(PAD + c + shift, SPAN), :]
                term = piece if term is None else term + piece
            high = term.astype(jnp.bfloat16)
            low = (term - high.astype(jnp.float32)).astype(jnp.bfloat16)
            part = lax.dot_general(ones, jnp.concatenate([high, low], axis=1), (((1,), (1,)), ((), ())),
                                   preferred_element_type=jnp.float32)
            store(pl.ds(c, SPAN), part[0:1])

    def add_link(k, r, row, shift, hs):
        def store(at, part):
            sums[k, pl.ds(r - first, 1), at] = part
        link(r - first + 1, row - first + 1, shift, hs, store)

    def along(r, carry):
        add_link(0, r, r, -1, both)
        add_link(1, r, r, 1, both)
        return carry

    def across(r, carry):
        add_link(3, r, r + 1, 0, both)
        add_link(2, r + 1, r, 0, both)
        return carry

    def outer(halo):
        r0 = jnp.where(halo == 0, first - HALO, last + HALO)
        step = jnp.where(halo == 0, 1, -1)

        def diagonal(s, carry):
            relax(r0 + step * s, s, (halo,))
            return carry
        lax.fori_loop(1, STEPS + 1, diagonal, 0)

    scale = 1.0 / (m * halves * LANES)

    def cross(halo):
        there = jnp.where(halo == 0, has_top, has_bottom)
        r0 = jnp.where(halo == 0, first - HALO, last + HALO)
        step = jnp.where(halo == 0, 1, -1)
        own = jnp.where(halo == 0, 1, rows)
        other = jnp.where(halo == 0, 0, rows + 1)
        arrive_outer(halo)

        @pl.when(there)
        def _():
            base = (me * rows + r0 - first) * cols
            names, wants = anchors[halo], demand[halo]
            for i in range(cols // CHUNK):
                at, mine = pl.ds(PAD + i * CHUNK, CHUNK), pl.ds(i * CHUNK, CHUNK)
                node = lax.broadcasted_iota(jnp.int32, (CHUNK, LANES), 0) + (base + i * CHUNK)
                value = jnp.where(node == names, 0.0, tail[halo, halves, mine, :])
                for t in range(1, STEPS + 1):
                    value = value + wide[2 + halo, r0 + step * t - 1, mine, :]
                power = jnp.minimum(value, grid[STEPS % 2, halo, r0 + step * STEPS, at, :]) * RATE
                decay[halo, other, at, :] = jnp.exp2(-power)
                growth[halo, other, mine, :] = wants * jnp.exp2(power)

            def mine_store(at, part):
                sums[2 + halo, pl.ds(own - 1, 1), at] = part
            link(own, other, 0, (halo,), mine_store)

            def near_store(at, part):
                value = part * fees[4 + halo, pl.ds(jnp.where(halo == 0, rows - 1, 0), 1), at]
                for c in range(0, at.size, width):
                    near_out[halo, (at.start + c) // width] = value[:, c:c + width]
            link(other, own, 0, (halo,), near_store)
            for p in range(m):
                near_copy(halo, p).start()

    def near_copy(halo, p):
        return pltpu.make_async_remote_copy(
            src_ref=near_out.at[halo, p], dst_ref=near_in.at[1 - halo, org], send_sem=near_send.at[halo, p],
            recv_sem=near_recv.at[1 - halo, org],
            device_id={"blk": jnp.where(halo == 0, top, bottom), "org": p}, device_id_type=MESH)

    def near_wait(halo, p):
        pltpu.make_async_remote_copy(
            src_ref=near_out.at[halo, p], dst_ref=near_in.at[halo, p], send_sem=near_send.at[halo, p],
            recv_sem=near_recv.at[halo, p], device_id={"blk": sides[halo][1], "org": p}, device_id_type=MESH).wait_recv()

    def ahead(halo):
        def diagonal(s, carry):
            relax(jnp.where(halo == 0, first - STEPS + s, last + STEPS - s), s, both)
            return carry
        lax.fori_loop(1, STEPS + 1, diagonal, 0)

    def chain(halo, h, kept):
        there = jnp.where(halo == 0, has_top, has_bottom)
        r0 = jnp.where(halo == 0, first - STEPS, last + STEPS)
        step = jnp.where(halo == 0, 1, -1)
        q = jnp.where(halo == 0, 0, rows - 1)
        arrive(halo, STEPS, h)

        @pl.when(there)
        def _():
            base = (me * rows + r0 - first) * cols
            for i in range(cols // CHUNK):
                at, mine = pl.ds(PAD + i * CHUNK, CHUNK), pl.ds(i * CHUNK, CHUNK)
                node = lax.broadcasted_iota(jnp.int32, (CHUNK, LANES), 0) + (base + i * CHUNK)
                value = jnp.where(node == anchors[h], 0.0, tail[halo, h, mine, :])
                if kept:
                    grid[0, h, r0, at, :] = value
                for t in range(1, STEPS + 1):
                    r = r0 + step * t
                    value = jnp.minimum(grid[t % 2, h, r, at, :], value + wide[2 + halo, r - 1, mine, :])
                    if kept or t == STEPS:
                        grid[t % 2, h, r, at, :] = value

        def settle(h_static):
            for i in range(cols // CHUNK):
                at, mine = pl.ds(PAD + i * CHUNK, CHUNK), pl.ds(i * CHUNK, CHUNK)
                value = grid[STEPS % 2, h_static, q + first, at, :]
                final[q, mine, pl.ds(h_static * LANES, LANES)] = value
                power = value * RATE
                decay[h_static, q + 1, at, :] = jnp.exp2(-power)
                growth[h_static, q + 1, mine, :] = demand[h_static] * jnp.exp2(power)
        for k in both:
            @pl.when(h == k)
            def _():
                settle(k)

    bulk = STEPS // 2

    def closing_side(q, carry):
        halo = pair(q)

        def near(j, carry):
            @pl.when(q == 0)
            def _():
                forward(j)
            closing(halo, j)

            @pl.when(q == 1)
            def _():
                edge_links(j)
            return carry
        lax.fori_loop(bulk + 1, STEPS, near, 0)

        @pl.when(q == 0)
        def _():
            forward(STEPS)
            forward(HALO)
        ahead(halo)
        chain(halo, halo, True)
        outer(halo)
        cross(halo)
        chain(halo, 1 - halo, False)

        @pl.when(q == 0)
        def _():
            low = jnp.where(late == 0, first + bulk, first)
            lax.fori_loop(low, low + rows - bulk, along, 0)
            lax.fori_loop(low, low + rows - bulk - 1, across, 0)

        @pl.when(q == 1)
        def _():
            edge_links(STEPS)
        return carry

    def edge_links(j):
        r = jnp.where(late == 0, first - j + STEPS, last + j - STEPS)
        along(r, 0)
        across(r - late, 0)

    for k in range(4):
        fees[k] = jnp.exp(-temper * raw[0, k]) * scale
    for halo in range(2):
        fees[4 + halo] = jnp.exp(-temper * raw[1 + halo, 3 - halo]) * scale

    lax.fori_loop(1, bulk, opening, 0)
    for from_plane, via_plane, moved in plans:
        @pl.when(paired & (org == via_plane))
        def _():
            pltpu.make_async_remote_copy(
                src_ref=lend.at[pl.ds(0, moved)], dst_ref=lend.at[pl.ds(0, moved)], send_sem=lend_out.at[0],
                recv_sem=lend_in.at[0], device_id={"org": from_plane}, device_id_type=MESH).wait_recv()
            lend_on(from_plane, moved).start()
    forward(bulk)
    for q in range(2):
        closing(pair(q), bulk)
    lax.fori_loop(0, 2, closing_side, 0)

    for p in range(m):
        share[p] = sums[:, :, p * width:(p + 1) * width] * fees[0:4, :, p * width:(p + 1) * width]

    def org_copy(d):
        peer = lax.rem(org + d, m)
        return pltpu.make_async_remote_copy(
            src_ref=share.at[peer], dst_ref=landed.at[d - 1], send_sem=org_send.at[d - 1], recv_sem=org_recv.at[d - 1],
            device_id={"org": peer}, device_id_type=MESH)
    for d in range(1, m):
        org_copy(d).start()
    for side in range(2):
        @pl.when(sides[side][0])
        def _():
            cost_copy(side).wait_send()
        @pl.when(sides[1 - side][0])
        def _():
            for d in range(1, m):
                cost_spread(side, d).wait_send()
    all_sends(lambda copy: copy.wait_send())
    for from_plane, via_plane, moved in plans:
        @pl.when(paired & (org == via_plane))
        def _():
            lend_on(from_plane, moved).wait_send()
    if relayed:
        for side in range(2):
            @pl.when(me == via[side])
            def _():
                def body(j, carry):
                    for h in both:
                        from_relay(side, j, h).wait_send()
                    return carry
                lax.fori_loop(1, STEPS, body, 0)
                body(STEPS, 0)
                from_relay(side, HALO, 1 - side).wait_send()
    for d in range(1, m):
        org_copy(d).wait_send()
    for side in range(2):
        @pl.when(sides[side][0])
        def _():
            for p in range(m):
                near_copy(side, p).wait_send()
    result = share[org]
    for d in range(1, m):
        org_copy(d).wait_recv()
        result += landed[d - 1]
    weights[...] = result
    for halo in range(2):
        @pl.when(sides[halo][0])
        def _():
            at = 0 if halo == 0 else rows - 1
            extra = weights[2 + halo, pl.ds(at, 1), :]
            for p in range(m):
                near_wait(halo, p)
                extra += near_in[halo, p]
            weights[2 + halo, pl.ds(at, 1), :] = extra


def leave(rows, labels, weights, labels_out, weights_out, sems):
    copies = [pltpu.make_async_copy(labels.at[r], labels_out.at[r], sems.at[r]) for r in range(rows)]
    copies.append(pltpu.make_async_copy(weights, weights_out, sems.at[rows]))
    for copy in copies:
        copy.start()
    for copy in copies:
        copy.wait()


def local(n, m, warm_labels, link_costs, anchor_nodes, demand):
    rows, cols, count = warm_labels.shape
    halves = count // LANES
    total = rows + 2 * HALO
    width = cols // m
    units = STEPS * halves + 1
    any_space = pl.BlockSpec(memory_space=pl.ANY)
    vmem = pl.BlockSpec(memory_space=pltpu.VMEM)
    dma = pltpu.SemaphoreType.DMA
    labels, weights = pl.pallas_call(
        functools.partial(kernel, n, m, rows, cols, halves),
        out_shape=(
            pltpu.VMEM((rows, cols, count), jnp.float32),
            pltpu.VMEM((4, rows, width), jnp.float32),
        ),
        in_specs=[any_space] * 4,
        out_specs=(vmem, vmem),
        scratch_shapes=[
            pltpu.VMEM((2, halves, total, cols + 2 * PAD, LANES), jnp.float32),
            pltpu.VMEM((4, total - 2, cols, LANES), jnp.float32),
            pltpu.VMEM((4, 4, rows, cols), jnp.float32),
            pltpu.VMEM((cols, 16 * rows), jnp.float32),
            pltpu.VMEM((halves, rows + 2, cols + 2 * PAD, LANES), jnp.float32),
            pltpu.VMEM((halves, rows + 2, cols, LANES), jnp.float32),
            pltpu.VMEM((2, halves + 1, cols, LANES), jnp.float32),
            pltpu.VMEM((units, cols - cols // 2, LANES), jnp.float32),
            pltpu.VMEM((4, rows, cols), jnp.float32),
            pltpu.VMEM((m, 4, rows, width), jnp.float32),
            pltpu.VMEM((max(m - 1, 1), 4, rows, width), jnp.float32),
            pltpu.VMEM((2, m, 1, width), jnp.float32),
            pltpu.VMEM((2, m, 1, width), jnp.float32),
            dma((2, units, 2)),
            dma((2, units, 2)),
            dma((units,)),
            dma((units,)),
            dma((2, m)),
            dma((2, m)),
            dma((max(m - 1, 1),)),
            dma((max(m - 1, 1),)),
            dma((2, m)),
            dma((2, m)),
            pltpu.VMEM((cols * 13 // 16, LANES), jnp.float32),
            dma((1,)),
            dma((1,)),
            dma((1,)),
            pltpu.SemaphoreType.REGULAR,
            pltpu.VMEM((halves, 1, LANES), jnp.int32),
            pltpu.VMEM((halves, 1, LANES), jnp.float32),
            pltpu.VMEM((6, rows, cols), jnp.float32),
            dma((halves + 3,)),
        ],
        compiler_params=pltpu.CompilerParams(collective_id=0, has_side_effects=True, vmem_limit_bytes=58 * 1024 * 1024),
    )(warm_labels, link_costs, anchor_nodes.reshape(halves, 1, LANES), demand.reshape(halves, 1, LANES))
    labels = pltpu.with_memory_space_constraint(labels, pltpu.VMEM)
    weights = pltpu.with_memory_space_constraint(weights, pltpu.VMEM)
    return pl.pallas_call(
        functools.partial(leave, rows),
        out_shape=(
            jax.ShapeDtypeStruct((rows, cols, count), jnp.float32),
            jax.ShapeDtypeStruct((4, rows, width), jnp.float32),
        ),
        in_specs=[vmem, vmem],
        out_specs=(any_space, any_space),
        scratch_shapes=[dma((rows + 1,))],
        compiler_params=pltpu.CompilerParams(vmem_limit_bytes=8 * 1024 * 1024),
    )(labels, weights)


def solution(mesh):
    placed = (P("blk", None, "org"), P(None, "blk", None), P("org"), P("org"))
    return jax.shard_map(
        functools.partial(local, mesh.shape["blk"], mesh.shape["org"]),
        mesh=mesh,
        in_specs=placed,
        out_specs=(P("blk", None, "org"), P(None, "blk", "org")),
        check_vma=False,
    )
```

```python
import functools
import math

import jax
import jax.numpy as jnp
from jax import lax
from jax.experimental import pallas as pl
from jax.experimental.pallas import tpu as pltpu
from jax.sharding import PartitionSpec as P

INNER = 2
ROUNDS = 3
STEPS = INNER * ROUNDS
HALO = STEPS + 1

far_value = 1000000000.0
temper = 0.5
RATE = temper * math.log2(math.e)
LANES = 128
PAD = 8
CHUNK = 32
BAND = 64
SPAN = 256
MESH = pl.DeviceIdType.MESH


def kernel(n, m, rows, cols, halves, warm, costs, anchors_in, demand_in, final, weights, grid, wide, raw, turned, decay, growth, tail,
           relay, sums, share, landed, near_out, near_in, row_send, row_recv, relay_in, relay_out, cost_send, cost_recv,
           org_send, org_recv, near_send, near_recv, lend, lend_in, lend_out, lend_recv, ready, anchors, demand, fees, local_sem):
    me = lax.axis_index("blk")
    org = lax.axis_index("org")
    has_top = me > 0
    has_bottom = me < n - 1
    top = jnp.maximum(me - 1, 0)
    bottom = jnp.minimum(me + 1, n - 1)
    first, last = HALO, HALO + rows - 1
    total = rows + 2 * HALO
    inner = pl.ds(PAD, cols)
    sides = ((has_top, top), (has_bottom, bottom))
    mid = n // 2
    relayed = n == 8
    via = (0, n - 1)
    goal = (mid - 1, mid)
    splits = tuple(relayed and me == goal[1 - side] for side in range(2))
    cut = cols // 2
    width = cols // m
    late = lax.rem(me, 2)
    early = 1 - late
    last_unit = STEPS * halves
    plans = ((m - 1, 0, cols * 13 // 16), (m - 2, 1, cols * 9 // 32)) if relayed and m == 4 else ()
    paired = (me != 0) & (me != n - 1) & (me != mid - 1) & (me != mid)

    barrier = pltpu.get_barrier_semaphore()
    for there, who in sides:
        @pl.when(there)
        def _():
            pl.semaphore_signal(barrier, inc=1, device_id={"blk": who}, device_id_type=MESH)

    def greet(signal, p):
        pl.semaphore_signal(signal, inc=1, device_id={"org": p}, device_id_type=MESH)
        for there, who in sides:
            @pl.when(there)
            def _():
                pl.semaphore_signal(signal, inc=1, device_id={"blk": who, "org": p}, device_id_type=MESH)
    for p in range(1, m):
        @pl.when(org < p)
        def _():
            greet(barrier, p)
    if relayed:
        for a, b in ((mid - 1, 0), (mid - 1, n - 1), (mid, 0), (mid, n - 1)):
            for mine, other in ((a, b), (b, a)):
                @pl.when(me == mine)
                def _():
                    pl.semaphore_signal(barrier, inc=1, device_id={"blk": other}, device_id_type=MESH)
    own_cost = pltpu.make_async_copy(costs, raw.at[0], local_sem.at[halves])
    own_cost.start()
    listed = (pltpu.make_async_copy(anchors_in, anchors, local_sem.at[halves + 1]),
              pltpu.make_async_copy(demand_in, demand, local_sem.at[halves + 2]))
    for copy in listed:
        copy.start()

    def own_rows(h):
        return pltpu.make_async_copy(
            warm.at[:, :, pl.ds(h * LANES, LANES)],
            grid.at[0, h, pl.ds(first, rows), inner, :],
            local_sem.at[h])
    for h in range(halves):
        own_rows(h).start()
    around = jnp.where(has_top, 1, 0) + jnp.where(has_bottom, 1, 0)
    pl.semaphore_wait(barrier, around + org * (1 + around)
                      + (jnp.where((me == 0) | (me == n - 1) | (me == mid) | (me == mid - 1), 2, 0) if relayed else 0))

    part = 4 // m
    piece_of = pl.ds(org * part, part)

    def cost_copy(side):
        return pltpu.make_async_remote_copy(
            src_ref=costs.at[piece_of], dst_ref=raw.at[2 - side, piece_of], send_sem=cost_send.at[side, 0],
            recv_sem=cost_recv.at[side, 0], device_id={"blk": sides[side][1]}, device_id_type=MESH)

    def cost_spread(side, d):
        return pltpu.make_async_remote_copy(
            src_ref=raw.at[2 - side, piece_of], dst_ref=raw.at[2 - side, piece_of], send_sem=cost_send.at[side, d],
            recv_sem=cost_recv.at[side, d], device_id={"org": lax.rem(org + d, m)}, device_id_type=MESH)

    def source(side, j, h, start, count):
        row = jnp.where(side == 0, j - 1, rows - j)
        return warm.at[row, pl.ds(start, count), pl.ds(h * LANES, LANES)]

    def target(side, j, h, start, count):
        if isinstance(j, int) and j >= STEPS:
            return tail.at[1 - side, halves if j == HALO else h, pl.ds(start, count), :]
        row = jnp.where(side == 0, last + j, first - j)
        return grid.at[0, h, row, pl.ds(PAD + start, count), :]

    def unit(j, h):
        return last_unit if isinstance(j, int) and j == HALO else (j - 1) * halves + h

    def row_copy(side, j, h, count):
        u = unit(j, h)
        return pltpu.make_async_remote_copy(
            src_ref=source(side, j, h, 0, count), dst_ref=target(side, j, h, 0, count),
            send_sem=row_send.at[side, u, 0], recv_sem=row_recv.at[side, u, 0],
            device_id={"blk": jnp.where(side == 0, top, bottom)}, device_id_type=MESH)

    def to_relay(side, j, h):
        u = unit(j, h)
        return pltpu.make_async_remote_copy(
            src_ref=source(side, j, h, cut, cols - cut), dst_ref=relay.at[u],
            send_sem=row_send.at[side, u, 1], recv_sem=relay_in.at[u],
            device_id={"blk": via[side]}, device_id_type=MESH)

    def from_relay(side, j, h):
        u = unit(j, h)
        return pltpu.make_async_remote_copy(
            src_ref=relay.at[u], dst_ref=target(side, j, h, cut, cols - cut),
            send_sem=relay_out.at[u], recv_sem=row_recv.at[side, u, 1],
            device_id={"blk": goal[side]}, device_id_type=MESH)

    def each_send(j, h, side, act):
        there, split = sides[side][0], splits[side]
        @pl.when(there & jnp.logical_not(split) if relayed else there)
        def _():
            act(row_copy(side, j, h, cols))
        if relayed:
            @pl.when(split)
            def _():
                act(to_relay(side, j, h))
                act(row_copy(side, j, h, cut))

    def lend_copy(side, via_plane, moved):
        kept = cols - moved
        return pltpu.make_async_remote_copy(
            src_ref=source(side, HALO, 1 - side, kept, moved), dst_ref=lend.at[pl.ds(0, moved)],
            send_sem=row_send.at[side, last_unit, 1], recv_sem=lend_in.at[0],
            device_id={"blk": sides[side][1], "org": via_plane}, device_id_type=MESH)

    def lend_on(from_plane, moved):
        return pltpu.make_async_remote_copy(
            src_ref=lend.at[pl.ds(0, moved)], dst_ref=tail.at[late, halves, pl.ds(cols - moved, moved), :],
            send_sem=lend_out.at[0], recv_sem=lend_recv.at[0], device_id={"org": from_plane}, device_id_type=MESH)

    def outer_send(side, act):
        there, split = sides[side][0], splits[side]
        lending = paired & (late == side)
        plain = there
        for from_plane, via_plane, moved in plans:
            here = lending & (org == from_plane)
            plain = plain & jnp.logical_not(here)

            @pl.when(here)
            def _():
                act(row_copy(side, HALO, 1 - side, cols - moved))
                act(lend_copy(side, via_plane, moved))

        @pl.when(plain & jnp.logical_not(split) if relayed else plain)
        def _():
            act(row_copy(side, HALO, 1 - side, cols))
        if relayed:
            @pl.when(split)
            def _():
                act(to_relay(side, HALO, 1 - side))
                act(row_copy(side, HALO, 1 - side, cut))

    def all_sends(act):
        def body(j, carry):
            for h in range(halves):
                for side in range(2):
                    each_send(j, h if side else halves - 1 - h, side, act)
            return carry
        lax.fori_loop(1, STEPS, body, 0)
        for side in range(2):
            each_send(STEPS, 1 - side, side, act)
        for side in range(2):
            outer_send(side, act)
        for side in range(2):
            each_send(STEPS, side, side, act)

    def arrive(halo, j, h):
        side = 1 - halo
        there = jnp.where(halo == 0, has_top, has_bottom)
        split = jnp.where(halo == 0, me == goal[1], me == goal[0]) & there
        @pl.when(there & jnp.logical_not(split) if relayed else there)
        def _():
            pltpu.make_async_remote_copy(
                src_ref=source(0, 1, 0, 0, cols), dst_ref=target(side, j, h, 0, cols),
                send_sem=row_send.at[side, unit(j, h), 0], recv_sem=row_recv.at[side, unit(j, h), 0],
                device_id={"blk": bottom}, device_id_type=MESH).wait_recv()
        if relayed:
            @pl.when(split)
            def _():
                for part, start, count in ((0, 0, cut), (1, cut, cols - cut)):
                    pltpu.make_async_remote_copy(
                        src_ref=source(0, 1, 0, start, count), dst_ref=target(side, j, h, start, count),
                        send_sem=row_send.at[side, unit(j, h), part], recv_sem=row_recv.at[side, unit(j, h), part],
                        device_id={"blk": bottom}, device_id_type=MESH).wait_recv()

    def arrive_outer(halo):
        lending = paired & (late == halo)
        plain = jnp.bool_(True)
        for from_plane, _, moved in plans:
            here = lending & (org == from_plane)
            plain = plain & jnp.logical_not(here)

            @pl.when(here)
            def _():
                pltpu.make_async_remote_copy(
                    src_ref=source(0, 1, 0, 0, cols - moved), dst_ref=target(1 - halo, HALO, halo, 0, cols - moved),
                    send_sem=row_send.at[1 - halo, last_unit, 0], recv_sem=row_recv.at[1 - halo, last_unit, 0],
                    device_id={"blk": bottom}, device_id_type=MESH).wait_recv()
                lend_on(from_plane, moved).wait_recv()

        @pl.when(plain)
        def _():
            arrive(halo, HALO, halo)

    def forward(j):
        if relayed:
            for side in range(2):
                @pl.when(me == via[side])
                def _():
                    for h in (1 - side, side)[:1 if isinstance(j, int) and j == HALO else 2]:
                        to_relay(side, j, h).wait_recv()
                        from_relay(side, j, h).start()

    for side in range(2):
        @pl.when(sides[side][0])
        def _():
            cost_copy(side).start()
    all_sends(lambda copy: copy.start())
    for p in range(m - 1):
        @pl.when(org > p)
        def _():
            greet(ready, p)

    edge = jnp.full((PAD, LANES), far_value, jnp.float32)
    zero_edge = jnp.zeros((PAD, LANES), jnp.float32)

    def fill_edges(r, carry):
        for b in range(2):
            for h in range(halves):
                grid[b, h, r, pl.ds(0, PAD), :] = edge
                grid[b, h, r, pl.ds(PAD + cols, PAD), :] = edge
        return carry
    lax.fori_loop(0, total, fill_edges, 0)

    def fill_decay(r, carry):
        for h in range(halves):
            decay[h, r, pl.ds(0, PAD), :] = zero_edge
            decay[h, r, pl.ds(PAD + cols, PAD), :] = zero_edge
        return carry
    lax.fori_loop(0, rows + 2, fill_decay, 0)
    sums[...] = jnp.zeros_like(sums)
    raw[3] = jnp.zeros_like(raw[3])

    def fill_row(r):
        for h in range(halves):
            grid[0, h, r, inner, :] = jnp.full((cols, LANES), far_value, jnp.float32)
    for r in (0, 1, total - 2, total - 1):
        fill_row(r)
    for missing, block, begin in ((me == 0, 1, 2), (me == n - 1, 2, last + 1)):
        @pl.when(missing)
        def _():
            raw[block] = jnp.full(raw.shape[1:], far_value, jnp.float32)
            def fill(r, carry):
                fill_row(begin + r)
                return carry
            lax.fori_loop(0, STEPS - 1, fill, 0)

    def place(r):
        base = (me * rows + r - first) * cols
        names = [anchors[h] for h in range(halves)]
        for i in range(cols // CHUNK):
            node = lax.broadcasted_iota(jnp.int32, (CHUNK, LANES), 0) + (base + i * CHUNK)
            at = pl.ds(PAD + i * CHUNK, CHUNK)
            for h in range(halves):
                grid[0, h, r, at, :] = jnp.where(node == names[h], 0.0, grid[0, h, r, at, :])

    @pl.when(org < m - 1)
    def _():
        pl.semaphore_wait(ready, (m - 1 - org) * (1 + around))
    for side in range(2):
        @pl.when(sides[1 - side][0])
        def _():
            cost_copy(side).wait_recv()
            for d in range(1, m):
                cost_spread(side, d).start()

    for copy in listed:
        copy.wait()
    for h in range(halves):
        own_rows(h).wait()

    def place_own(r, carry):
        place(r)
        return carry
    lax.fori_loop(first, last + 1, place_own, 0)

    own_cost.wait()
    for side in range(2):
        @pl.when(sides[1 - side][0])
        def _():
            for d in range(1, m):
                cost_spread(side, d).wait_recv()
    turned[...] = jnp.transpose(raw[...].reshape(4 * 4 * rows, cols))

    def widen(i, carry):
        at = pl.ds(pl.multiple_of(i * BAND, BAND), BAND)
        piece = turned[at, :]
        for r in range(1, total - 1):
            if r < first:
                block, row = 1, rows - first + r
            elif r <= last:
                block, row = 0, r - first
            else:
                block, row = 2, r - last - 1
            for k in range(4):
                lane = (block * 4 + k) * rows + row
                wide[k, r - 1, at, :] = jnp.broadcast_to(piece[:, lane:lane + 1], (BAND, LANES))
        return carry
    lax.fori_loop(0, cols // BAND, widen, 0)

    def best_of(old, r, i, hs):
        c0 = PAD + i * CHUNK
        at, mine = pl.ds(c0, CHUNK), pl.ds(i * CHUNK, CHUNK)
        price = [wide[k, r - 1, mine, :] for k in range(4)]
        result = []
        for h in hs:
            best = grid[old, h, r, at, :]
            best = jnp.minimum(best, grid[old, h, r, pl.ds(c0 - 1, CHUNK), :] + price[0])
            best = jnp.minimum(best, grid[old, h, r, pl.ds(c0 + 1, CHUNK), :] + price[1])
            best = jnp.minimum(best, grid[old, h, r - 1, at, :] + price[2])
            best = jnp.minimum(best, grid[old, h, r + 1, at, :] + price[3])
            result.append(best)
        return at, mine, result

    def relax(r, s, hs):
        old, new = lax.rem(s + 1, 2), lax.rem(s, 2)
        for i in range(cols // CHUNK):
            at, _, result = best_of(old, r, i, hs)
            for h, best in zip(hs, result):
                grid[new, h, r, at, :] = best

    both = tuple(range(halves))

    def finish(halo, j):
        r = jnp.where(halo == 0, first - j + STEPS, last + j - STEPS)
        q = r - first
        wants = [demand[h] for h in both]
        for i in range(cols // CHUNK):
            at, mine, result = best_of((STEPS + 1) % 2, r, i, both)
            for h, best in zip(both, result):
                final[q, mine, pl.ds(h * LANES, LANES)] = best
                power = best * RATE
                decay[h, q + 1, at, :] = jnp.exp2(-power)
                growth[h, q + 1, mine, :] = wants[h] * jnp.exp2(power)

    middle = rows // 2
    for s in range(1, middle):
        def inside(r, carry):
            relax(r, jnp.int32(s), both)
            return carry
        lax.fori_loop(first + s, last - s + 1, inside, 0)

    def stage(halo, j):
        for h in both:
            arrive(halo, j, h)
        place(jnp.where(halo == 0, first - j, last + j))

        def diagonal(s, carry):
            relax(jnp.where(halo == 0, first - j + s, last + j - s), s, both)
            return carry
        lax.fori_loop(1, jnp.minimum(STEPS - 1, j + middle - 1) + 1, diagonal, 0)

    def pair(q):
        return jnp.where(q == 0, early, late)

    def opening(j, carry):
        forward(j)

        def one(q, carry):
            stage(pair(q), j)
            return carry
        return lax.fori_loop(0, 2, one, carry)

    def closing(halo, j):
        stage(halo, j)
        finish(halo, j)

    ones = jnp.ones((8, 2 * LANES), jnp.bfloat16)

    def link(own, other, shift, hs, store):
        for c in range(0, cols, SPAN):
            term = None
            for h in hs:
                piece = growth[h, own, pl.ds(c, SPAN), :] * decay[h, other, pl.ds(PAD + c + shift, SPAN), :]
                term = piece if term is None else term + piece
            high = term.astype(jnp.bfloat16)
            low = (term - high.astype(jnp.float32)).astype(jnp.bfloat16)
            part = lax.dot_general(ones, jnp.concatenate([high, low], axis=1), (((1,), (1,)), ((), ())),
                                   preferred_element_type=jnp.float32)
            store(pl.ds(c, SPAN), part[0:1])

    def add_link(k, r, row, shift, hs):
        def store(at, part):
            sums[k, pl.ds(r - first, 1), at] = part
        link(r - first + 1, row - first + 1, shift, hs, store)

    def along(r, carry):
        add_link(0, r, r, -1, both)
        add_link(1, r, r, 1, both)
        return carry

    def across(r, carry):
        add_link(3, r, r + 1, 0, both)
        add_link(2, r + 1, r, 0, both)
        return carry

    def outer(halo):
        r0 = jnp.where(halo == 0, first - HALO, last + HALO)
        step = jnp.where(halo == 0, 1, -1)

        def diagonal(s, carry):
            relax(r0 + step * s, s, (halo,))
            return carry
        lax.fori_loop(1, STEPS + 1, diagonal, 0)

    scale = 1.0 / (m * halves * LANES)

    def cross(halo):
        there = jnp.where(halo == 0, has_top, has_bottom)
        r0 = jnp.where(halo == 0, first - HALO, last + HALO)
        step = jnp.where(halo == 0, 1, -1)
        own = jnp.where(halo == 0, 1, rows)
        other = jnp.where(halo == 0, 0, rows + 1)
        arrive_outer(halo)

        @pl.when(there)
        def _():
            base = (me * rows + r0 - first) * cols
            names, wants = anchors[halo], demand[halo]
            for i in range(cols // CHUNK):
                at, mine = pl.ds(PAD + i * CHUNK, CHUNK), pl.ds(i * CHUNK, CHUNK)
                node = lax.broadcasted_iota(jnp.int32, (CHUNK, LANES), 0) + (base + i * CHUNK)
                value = jnp.where(node == names, 0.0, tail[halo, halves, mine, :])
                for t in range(1, STEPS + 1):
                    value = value + wide[2 + halo, r0 + step * t - 1, mine, :]
                power = jnp.minimum(value, grid[STEPS % 2, halo, r0 + step * STEPS, at, :]) * RATE
                decay[halo, other, at, :] = jnp.exp2(-power)
                growth[halo, other, mine, :] = wants * jnp.exp2(power)

            def mine_store(at, part):
                sums[2 + halo, pl.ds(own - 1, 1), at] = part
            link(own, other, 0, (halo,), mine_store)

            def near_store(at, part):
                value = part * fees[4 + halo, pl.ds(jnp.where(halo == 0, rows - 1, 0), 1), at]
                for c in range(0, at.size, width):
                    near_out[halo, (at.start + c) // width] = value[:, c:c + width]
            link(other, own, 0, (halo,), near_store)
            for p in range(m):
                near_copy(halo, p).start()

    def near_copy(halo, p):
        return pltpu.make_async_remote_copy(
            src_ref=near_out.at[halo, p], dst_ref=near_in.at[1 - halo, org], send_sem=near_send.at[halo, p],
            recv_sem=near_recv.at[1 - halo, org],
            device_id={"blk": jnp.where(halo == 0, top, bottom), "org": p}, device_id_type=MESH)

    def near_wait(halo, p):
        pltpu.make_async_remote_copy(
            src_ref=near_out.at[halo, p], dst_ref=near_in.at[halo, p], send_sem=near_send.at[halo, p],
            recv_sem=near_recv.at[halo, p], device_id={"blk": sides[halo][1], "org": p}, device_id_type=MESH).wait_recv()

    def ahead(halo):
        def diagonal(s, carry):
            relax(jnp.where(halo == 0, first - STEPS + s, last + STEPS - s), s, both)
            return carry
        lax.fori_loop(1, STEPS + 1, diagonal, 0)

    def chain(halo, h, kept):
        there = jnp.where(halo == 0, has_top, has_bottom)
        r0 = jnp.where(halo == 0, first - STEPS, last + STEPS)
        step = jnp.where(halo == 0, 1, -1)
        q = jnp.where(halo == 0, 0, rows - 1)
        arrive(halo, STEPS, h)

        @pl.when(there)
        def _():
            base = (me * rows + r0 - first) * cols
            for i in range(cols // CHUNK):
                at, mine = pl.ds(PAD + i * CHUNK, CHUNK), pl.ds(i * CHUNK, CHUNK)
                node = lax.broadcasted_iota(jnp.int32, (CHUNK, LANES), 0) + (base + i * CHUNK)
                value = jnp.where(node == anchors[h], 0.0, tail[halo, h, mine, :])
                if kept:
                    grid[0, h, r0, at, :] = value
                for t in range(1, STEPS + 1):
                    r = r0 + step * t
                    value = jnp.minimum(grid[t % 2, h, r, at, :], value + wide[2 + halo, r - 1, mine, :])
                    if kept or t == STEPS:
                        grid[t % 2, h, r, at, :] = value

        def settle(h_static):
            for i in range(cols // CHUNK):
                at, mine = pl.ds(PAD + i * CHUNK, CHUNK), pl.ds(i * CHUNK, CHUNK)
                value = grid[STEPS % 2, h_static, q + first, at, :]
                final[q, mine, pl.ds(h_static * LANES, LANES)] = value
                power = value * RATE
                decay[h_static, q + 1, at, :] = jnp.exp2(-power)
                growth[h_static, q + 1, mine, :] = demand[h_static] * jnp.exp2(power)
        for k in both:
            @pl.when(h == k)
            def _():
                settle(k)

    bulk = STEPS // 2

    def closing_side(q, carry):
        halo = pair(q)

        def near(j, carry):
            @pl.when(q == 0)
            def _():
                forward(j)
            closing(halo, j)

            @pl.when(q == 1)
            def _():
                edge_links(j)
            return carry
        lax.fori_loop(bulk + 1, STEPS, near, 0)

        @pl.when(q == 0)
        def _():
            forward(STEPS)
            forward(HALO)
        ahead(halo)
        chain(halo, halo, True)
        outer(halo)
        cross(halo)
        chain(halo, 1 - halo, False)

        @pl.when(q == 0)
        def _():
            low = jnp.where(late == 0, first + bulk, first)
            lax.fori_loop(low, low + rows - bulk, along, 0)
            lax.fori_loop(low, low + rows - bulk - 1, across, 0)

        @pl.when(q == 1)
        def _():
            edge_links(STEPS)
        return carry

    def edge_links(j):
        r = jnp.where(late == 0, first - j + STEPS, last + j - STEPS)
        along(r, 0)
        across(r - late, 0)

    for k in range(4):
        fees[k] = jnp.exp(-temper * raw[0, k]) * scale
    for halo in range(2):
        fees[4 + halo] = jnp.exp(-temper * raw[1 + halo, 3 - halo]) * scale

    lax.fori_loop(1, bulk, opening, 0)
    for from_plane, via_plane, moved in plans:
        @pl.when(paired & (org == via_plane))
        def _():
            pltpu.make_async_remote_copy(
                src_ref=lend.at[pl.ds(0, moved)], dst_ref=lend.at[pl.ds(0, moved)], send_sem=lend_out.at[0],
                recv_sem=lend_in.at[0], device_id={"org": from_plane}, device_id_type=MESH).wait_recv()
            lend_on(from_plane, moved).start()
    forward(bulk)
    for q in range(2):
        closing(pair(q), bulk)
    lax.fori_loop(0, 2, closing_side, 0)

    for p in range(m):
        share[p] = sums[:, :, p * width:(p + 1) * width] * fees[0:4, :, p * width:(p + 1) * width]

    def org_copy(d):
        peer = lax.rem(org + d, m)
        return pltpu.make_async_remote_copy(
            src_ref=share.at[peer], dst_ref=landed.at[d - 1], send_sem=org_send.at[d - 1], recv_sem=org_recv.at[d - 1],
            device_id={"org": peer}, device_id_type=MESH)
    for d in range(1, m):
        org_copy(d).start()
    for side in range(2):
        @pl.when(sides[side][0])
        def _():
            cost_copy(side).wait_send()
        @pl.when(sides[1 - side][0])
        def _():
            for d in range(1, m):
                cost_spread(side, d).wait_send()
    all_sends(lambda copy: copy.wait_send())
    for from_plane, via_plane, moved in plans:
        @pl.when(paired & (org == via_plane))
        def _():
            lend_on(from_plane, moved).wait_send()
    if relayed:
        for side in range(2):
            @pl.when(me == via[side])
            def _():
                def body(j, carry):
                    for h in both:
                        from_relay(side, j, h).wait_send()
                    return carry
                lax.fori_loop(1, STEPS, body, 0)
                body(STEPS, 0)
                from_relay(side, HALO, 1 - side).wait_send()
    for d in range(1, m):
        org_copy(d).wait_send()
    for side in range(2):
        @pl.when(sides[side][0])
        def _():
            for p in range(m):
                near_copy(side, p).wait_send()
    result = share[org]
    for d in range(1, m):
        org_copy(d).wait_recv()
        result += landed[d - 1]
    weights[...] = result
    for halo in range(2):
        @pl.when(sides[halo][0])
        def _():
            at = 0 if halo == 0 else rows - 1
            extra = weights[2 + halo, pl.ds(at, 1), :]
            for p in range(m):
                near_wait(halo, p)
                extra += near_in[halo, p]
            weights[2 + halo, pl.ds(at, 1), :] = extra


def leave(rows, labels, weights, labels_out, weights_out, sems):
    copies = [pltpu.make_async_copy(labels, labels_out, sems.at[0]), pltpu.make_async_copy(weights, weights_out, sems.at[1])]
    for copy in copies:
        copy.start()
    for copy in copies:
        copy.wait()


def local(n, m, warm_labels, link_costs, anchor_nodes, demand):
    rows, cols, count = warm_labels.shape
    halves = count // LANES
    total = rows + 2 * HALO
    width = cols // m
    units = STEPS * halves + 1
    any_space = pl.BlockSpec(memory_space=pl.ANY)
    vmem = pl.BlockSpec(memory_space=pltpu.VMEM)
    dma = pltpu.SemaphoreType.DMA
    labels, weights = pl.pallas_call(
        functools.partial(kernel, n, m, rows, cols, halves),
        out_shape=(
            pltpu.VMEM((rows, cols, count), jnp.float32),
            pltpu.VMEM((4, rows, width), jnp.float32),
        ),
        in_specs=[any_space] * 4,
        out_specs=(vmem, vmem),
        scratch_shapes=[
            pltpu.VMEM((2, halves, total, cols + 2 * PAD, LANES), jnp.float32),
            pltpu.VMEM((4, total - 2, cols, LANES), jnp.float32),
            pltpu.VMEM((4, 4, rows, cols), jnp.float32),
            pltpu.VMEM((cols, 16 * rows), jnp.float32),
            pltpu.VMEM((halves, rows + 2, cols + 2 * PAD, LANES), jnp.float32),
            pltpu.VMEM((halves, rows + 2, cols, LANES), jnp.float32),
            pltpu.VMEM((2, halves + 1, cols, LANES), jnp.float32),
            pltpu.VMEM((units, cols - cols // 2, LANES), jnp.float32),
            pltpu.VMEM((4, rows, cols), jnp.float32),
            pltpu.VMEM((m, 4, rows, width), jnp.float32),
            pltpu.VMEM((max(m - 1, 1), 4, rows, width), jnp.float32),
            pltpu.VMEM((2, m, 1, width), jnp.float32),
            pltpu.VMEM((2, m, 1, width), jnp.float32),
            dma((2, units, 2)),
            dma((2, units, 2)),
            dma((units,)),
            dma((units,)),
            dma((2, m)),
            dma((2, m)),
            dma((max(m - 1, 1),)),
            dma((max(m - 1, 1),)),
            dma((2, m)),
            dma((2, m)),
            pltpu.VMEM((cols * 13 // 16, LANES), jnp.float32),
            dma((1,)),
            dma((1,)),
            dma((1,)),
            pltpu.SemaphoreType.REGULAR,
            pltpu.VMEM((halves, 1, LANES), jnp.int32),
            pltpu.VMEM((halves, 1, LANES), jnp.float32),
            pltpu.VMEM((6, rows, cols), jnp.float32),
            dma((halves + 3,)),
        ],
        compiler_params=pltpu.CompilerParams(collective_id=0, has_side_effects=True, vmem_limit_bytes=58 * 1024 * 1024),
    )(warm_labels, link_costs, anchor_nodes.reshape(halves, 1, LANES), demand.reshape(halves, 1, LANES))
    labels = pltpu.with_memory_space_constraint(labels, pltpu.VMEM)
    weights = pltpu.with_memory_space_constraint(weights, pltpu.VMEM)
    return pl.pallas_call(
        functools.partial(leave, rows),
        out_shape=(
            jax.ShapeDtypeStruct((rows, cols, count), jnp.float32),
            jax.ShapeDtypeStruct((4, rows, width), jnp.float32),
        ),
        in_specs=[vmem, vmem],
        out_specs=(any_space, any_space),
        scratch_shapes=[dma((2,))],
        compiler_params=pltpu.CompilerParams(vmem_limit_bytes=8 * 1024 * 1024),
    )(labels, weights)


def solution(mesh):
    placed = (P("blk", None, "org"), P(None, "blk", None), P("org"), P("org"))
    return jax.shard_map(
        functools.partial(local, mesh.shape["blk"], mesh.shape["org"]),
        mesh=mesh,
        in_specs=placed,
        out_specs=(P("blk", None, "org"), P(None, "blk", "org")),
        check_vma=False,
    )
```
